128 devices in a mesh: data: 128 (over z, y, x, core).
Axes of the slice: x: 4, y: 4, z: 4, core: 2. Of those that a mesh axis runs over, the one named last changes fastest.
Arguments:
- x_tokens: bfloat16 [131072, 384], P('data')
- labels: int32 [3, 131072], P(None, 'data')
- w_up: bfloat16 [4, 384, 1536], replicated
- w_down: bfloat16 [4, 1536, 384], replicated
- task_heads: bfloat16 [3, 384, 13], replicated
Outputs:
- output 1: float32 [3], replicated
- output 2: float32 [3, 3], replicated
- output 3: float32 [4, 589824], P(None, 'data')
- output 4: float32 [4, 589824], P(None, 'data')
All inputs are finite; a program needn't handle non-finite values.
Results may differ from the reference program's by a relative error of at most 0.001.
Values are sent between devices in bfloat16 or wider.
A program may use at most 1 GiB of HBM per device.

```python
import jax
import jax.numpy as jnp
from jax import lax

D_MODEL = 384
D_FF = 1536
NUM_TASKS = 3
NUM_CLASSES = 13
NUM_LAYERS = 4
TOK_DEV = 1024
NUM_DEV = 128
EG_STEPS = 20


def setup_inputs(seed: int = 0) -> dict:
    base_key = jax.random.key(seed)
    sub_keys = jax.random.split(base_key, 10)
    num_tokens = NUM_DEV * TOK_DEV
    x_tokens = jax.random.normal(sub_keys[0], (num_tokens, D_MODEL), jnp.float32).astype(jnp.bfloat16)
    w_up = (jax.random.normal(sub_keys[1], (NUM_LAYERS, D_MODEL, D_FF), jnp.float32) * D_MODEL ** -0.5).astype(jnp.bfloat16)
    w_down = (jax.random.normal(sub_keys[2], (NUM_LAYERS, D_FF, D_MODEL), jnp.float32) * D_FF ** -0.5).astype(jnp.bfloat16)
    shared_head = jax.random.normal(sub_keys[3], (D_MODEL, NUM_CLASSES), jnp.float32)
    head_noise = jax.random.normal(sub_keys[4], (NUM_TASKS, D_MODEL, NUM_CLASSES), jnp.float32)
    task_order = jax.random.permutation(sub_keys[5], NUM_TASKS)
    task_sign = jnp.where(task_order < NUM_TASKS // 2, -1.0, 1.0)
    task_heads = ((task_sign[:, None, None] * shared_head[None] + 0.6 * head_noise) * D_MODEL ** -0.5).astype(jnp.bfloat16)
    dev_shift = jax.random.randint(sub_keys[6], (NUM_DEV, 1), 0, NUM_CLASSES)
    local_lab = jax.random.randint(sub_keys[7], (NUM_DEV, TOK_DEV), 0, max(NUM_CLASSES // 2, 1))
    base_lab = ((local_lab + dev_shift) % NUM_CLASSES).reshape(1, num_tokens)
    free_lab = jax.random.randint(sub_keys[8], (NUM_TASKS, num_tokens), 0, NUM_CLASSES)
    free_pick = jax.random.randint(sub_keys[9], (NUM_TASKS, num_tokens), 0, 4)
    labels = jnp.where(free_pick == 0, free_lab, base_lab).astype(jnp.int32)
    return {'x_tokens': x_tokens, 'labels': labels, 'w_up': w_up, 'w_down': w_down, 'task_heads': task_heads}


def simplex_weights(gram_mat):
    temperature = jnp.trace(gram_mat) / NUM_TASKS
    alpha_vec = jnp.full((NUM_TASKS,), 1.0 / NUM_TASKS, jnp.float32)
    for step_idx in range(EG_STEPS):
        grad_pull = jnp.sum(gram_mat * alpha_vec[None, :], axis=1)
        alpha_vec = alpha_vec * jnp.exp(-grad_pull / temperature)
        alpha_vec = alpha_vec / jnp.sum(alpha_vec)
    return alpha_vec


def block_grads(x_block, lab_block, w_up, w_down, task_heads):
    hidden = x_block
    saved_acts = []
    for layer_idx in range(NUM_LAYERS):
        pre_act = jnp.dot(hidden, w_up[layer_idx], preferred_element_type=jnp.float32)
        act_val, gelu_slope = jax.jvp(jax.nn.gelu, (pre_act,), (jnp.ones_like(pre_act),))
        act_bf = act_val.astype(jnp.bfloat16)
        mlp_out = jnp.dot(act_bf, w_down[layer_idx], preferred_element_type=jnp.float32)
        saved_acts.append((hidden, act_bf, gelu_slope))
        hidden = (hidden.astype(jnp.float32) + mlp_out).astype(jnp.bfloat16)
    heads_f = task_heads.astype(jnp.float32)
    logits = jnp.einsum('bd,tdc->tbc', hidden.astype(jnp.float32), heads_f)
    soft_probs = jax.nn.softmax(logits, axis=-1)
    onehot = (lab_block[:, :, None] == jnp.arange(NUM_CLASSES)[None, None, :]).astype(jnp.float32)
    head_err = (soft_probs - onehot).astype(jnp.bfloat16)
    d_hidden = jnp.einsum('tbc,tdc->tbd', head_err.astype(jnp.float32), heads_f).astype(jnp.bfloat16)
    up_list = []
    down_list = []
    for layer_idx in range(NUM_LAYERS - 1, -1, -1):
        hidden_in, act_bf, gelu_slope = saved_acts[layer_idx]
        d_hid_f = d_hidden.astype(jnp.float32)
        down_list.append(jnp.einsum('bf,tbd->tfd', act_bf.astype(jnp.float32), d_hid_f))
        d_act = jnp.einsum('tbd,fd->tbf', d_hid_f, w_down[layer_idx].astype(jnp.float32))
        d_pre = (d_act * gelu_slope[None]).astype(jnp.bfloat16)
        d_pre_f = d_pre.astype(jnp.float32)
        up_list.append(jnp.einsum('bd,tbf->tdf', hidden_in.astype(jnp.float32), d_pre_f))
        if layer_idx > 0:
            d_hidden = (d_hid_f + jnp.einsum('tbf,df->tbd', d_pre_f, w_up[layer_idx].astype(jnp.float32))).astype(jnp.bfloat16)
    return jnp.stack(up_list[::-1]), jnp.stack(down_list[::-1])


def reference(x_tokens, labels, w_up, w_down, task_heads):
    x_blocks = x_tokens.reshape(NUM_DEV, TOK_DEV, D_MODEL)
    lab_blocks = jnp.transpose(labels.reshape(NUM_TASKS, NUM_DEV, TOK_DEV), (1, 0, 2))
    zero_up = jnp.zeros((NUM_LAYERS, NUM_TASKS, D_MODEL, D_FF), jnp.float32)
    zero_down = jnp.zeros((NUM_LAYERS, NUM_TASKS, D_FF, D_MODEL), jnp.float32)

    def scan_body(running, token_block):
        up_grads, down_grads = block_grads(token_block[0], token_block[1], w_up, w_down, task_heads)
        return (running[0] + up_grads, running[1] + down_grads), None

    totals, unused = lax.scan(scan_body, (zero_up, zero_down), (x_blocks, lab_blocks))
    inv_tokens = 1.0 / (NUM_DEV * TOK_DEV)
    flat_up = (totals[0] * inv_tokens).reshape(NUM_LAYERS, NUM_TASKS, D_MODEL * D_FF)
    flat_down = (totals[1] * inv_tokens).reshape(NUM_LAYERS, NUM_TASKS, D_FF * D_MODEL)
    gram_mat = jnp.einsum('lts,lus->tu', flat_up, flat_up) + jnp.einsum('lts,lus->tu', flat_down, flat_down)
    task_weights = simplex_weights(gram_mat)
    grad_up = jnp.einsum('t,lts->ls', task_weights, flat_up)
    grad_down = jnp.einsum('t,lts->ls', task_weights, flat_down)
    return (task_weights, gram_mat, grad_up, grad_down)
```

```python
import functools

import jax
import jax.numpy as jnp
from jax import lax
from jax.experimental import pallas as pl
from jax.experimental.pallas import tpu as pltpu
from jax.sharding import PartitionSpec as P

EG_STEPS = 20
NT = 3
NL = 4
DM = 384
DF = 1536
TOK = 1024
UNITS = NT * NL
AXIS_STRIDE = (2, 8, 32)
MESH = pl.DeviceIdType.MESH
F32 = jnp.float32
BF16 = jnp.bfloat16


def simplex_weights(gram_mat):
    num_tasks = gram_mat.shape[0]
    value_a11 = jnp.trace(gram_mat) / num_tasks
    alpha_vec = jnp.full((num_tasks,), 1.0 / num_tasks, jnp.float32)
    for step_idx in range(EG_STEPS):
        grad_pull = jnp.sum(gram_mat * alpha_vec[None, :], axis=1)
        alpha_vec = alpha_vec * jnp.exp(-grad_pull / value_a11)
        alpha_vec = alpha_vec / jnp.sum(alpha_vec)
    return alpha_vec


def half_slice(half):
    return slice(None) if half is None else pl.ds(2 * half, 2)


def backward_kernel(*refs):
    (at0, at1, at2, at3, ht0, ht1, ht2, ht3, sl0, sl1, sl2, sl3,
     w1t_hbm, w2t_hbm, d0_hbm, out_ref,
     at, ht, sl, w1t, w2t, dbuf, sbuf, tmp,
     gown, gsend, rd2d, ra1, rb1, acc2, ra2, rb2, acc3, r3,
     load_sem, d_sem, d2d_s, d2d_r, a1_s, a1_r, b1_s, b1_r,
     a2_s, a2_r, b2_s, b2_r, c3_s, c3_r) = refs
    at_hbm, ht_hbm, sl_hbm = (at0, at1, at2, at3), (ht0, ht1, ht2, ht3), (sl0, sl1, sl2, sl3)

    me = lax.axis_index('data')
    core = lax.rem(me, 2)
    pos = [lax.rem(me // s, 4) for s in AXIS_STRIDE]
    sibling = me + 1 - 2 * core

    def at_pos(axis, k):
        return lax.rem(pos[axis] + k, 4)

    def peer(axis, k):
        return me + (at_pos(axis, k) - pos[axis]) * AXIS_STRIDE[axis]

    barrier = pltpu.get_barrier_semaphore()
    partners = [sibling] + [peer(a, k) for a in range(3) for k in (1, 2, 3)]
    for dev in partners:
        pl.semaphore_signal(barrier, inc=1, device_id=(dev,), device_id_type=MESH)

    def loads(layer, slot):
        return [
            pltpu.make_async_copy(at_hbm[layer], at.at[slot], load_sem.at[0, slot]),
            pltpu.make_async_copy(ht_hbm[layer], ht.at[slot], load_sem.at[1, slot]),
            pltpu.make_async_copy(sl_hbm[layer], sl.at[slot], load_sem.at[2, slot]),
            pltpu.make_async_copy(w1t_hbm.at[layer], w1t.at[slot], load_sem.at[3, slot]),
            pltpu.make_async_copy(w2t_hbm.at[layer], w2t.at[slot], load_sem.at[4, slot]),
        ]

    d_load = pltpu.make_async_copy(d0_hbm, dbuf, d_sem)
    d_load.start()
    for cp in loads(NL - 1, 0):
        cp.start()
    pl.semaphore_wait(barrier, len(partners))
    d_load.wait()

    def remote(src, dst, send, recv, dev):
        return pltpu.make_async_remote_copy(
            src_ref=src, dst_ref=dst, send_sem=send, recv_sem=recv,
            device_id=(dev,), device_id_type=MESH)

    def chunk1(g3, p, idx, half=None):
        h, rows = half_slice(half), pl.ds(24 * p, 24)
        return (gown.at[g3, h, :, idx, rows, :], gown.at[g3, h, idx, :, rows, :],
                gown.at[g3, idx, h, :, rows, :])[p]

    def chunk2(par, p, idx, half=None):
        h = half_slice(half)
        return (acc2.at[par, 0, h, idx], acc2.at[par, 1, idx, h], acc2.at[par, 2, h, idx])[p]

    def d2d_copies(v):
        par = lax.rem(v, 2)
        return [remote(gsend.at[par], rd2d.at[par], d2d_s.at[par], d2d_r.at[par], sibling)]

    def relay1(v):
        par, g3 = lax.rem(v, 2), lax.rem(v, 3)
        return [remote(chunk1(g3, p, at_pos(p, 2), d), ra1.at[par, p, d], a1_s.at[par, p, d],
                       a1_r.at[par, p, d], peer(p, 1 + 2 * d)) for p in range(3) for d in range(2)]

    def main1(v):
        par, g3 = lax.rem(v, 2), lax.rem(v, 3)
        return [remote(chunk1(g3, p, at_pos(p, 1 + 2 * d)), rb1.at[par, p, d], b1_s.at[par, p, d],
                       b1_r.at[par, p, d], peer(p, 1 + 2 * d)) for p in range(3) for d in range(2)]

    def relay2(v):
        par = lax.rem(v, 2)
        return [remote(chunk2(par, p, at_pos((p + 1) % 3, 2), d), ra2.at[par, p, d], a2_s.at[par, p, d],
                       a2_r.at[par, p, d], peer((p + 1) % 3, 1 + 2 * d)) for p in range(3) for d in range(2)]

    def main2(v):
        par = lax.rem(v, 2)
        return [remote(chunk2(par, p, at_pos((p + 1) % 3, 1 + 2 * d)), rb2.at[par, p, d], b2_s.at[par, p, d],
                       b2_r.at[par, p, d], peer((p + 1) % 3, 1 + 2 * d)) for p in range(3) for d in range(2)]

    def last3(v):
        par = lax.rem(v, 2)
        return [remote(acc3.at[par, p, at_pos((p + 2) % 3, k)], r3.at[par, p, k - 1], c3_s.at[par, p, k - 1],
                       c3_r.at[par, p, k - 1], peer((p + 2) % 3, k)) for p in range(3) for k in (1, 2, 3)]

    def start(copies):
        for cp in copies:
            cp.start()

    def wait(copies):
        for cp in copies:
            cp.wait()

    def step_d2d(v):
        wait(d2d_copies(v))
        par, g3 = lax.rem(v, 2), lax.rem(v, 3)

        def add(i, carry):
            gown[g3, i] = gown[g3, i] + rd2d[par, i]
            return carry

        lax.fori_loop(0, 4, add, 0)
        start(relay1(v))

    def step_relay1(v):
        wait(relay1(v))
        par, g3 = lax.rem(v, 2), lax.rem(v, 3)
        for p in range(3):
            for d in range(2):
                dst = chunk1(g3, p, at_pos(p, 1 + 2 * d), d)
                dst[...] = dst[...] + ra1[par, p, d]
        start(main1(v))

    def step_main1(v):
        wait(main1(v))
        par, g3 = lax.rem(v, 2), lax.rem(v, 3)
        for p in range(3):
            acc2[par, p] = chunk1(g3, p, pos[p])[...] + rb1[par, p, 0] + rb1[par, p, 1]
        start(relay2(v))

    def step_relay2(v):
        wait(relay2(v))
        par = lax.rem(v, 2)
        for p in range(3):
            for d in range(2):
                dst = chunk2(par, p, at_pos((p + 1) % 3, 1 + 2 * d), d)
                dst[...] = dst[...] + ra2[par, p, d]
        start(main2(v))

    def step_main2(v):
        wait(main2(v))
        par = lax.rem(v, 2)
        for p in range(3):
            acc3[par, p] = chunk2(par, p, pos[(p + 1) % 3])[...] + rb2[par, p, 0] + rb2[par, p, 1]
        start(last3(v))

    def step_last3(v):
        wait(last3(v))
        par = lax.rem(v, 2)
        for p in range(3):
            out_ref[v, pl.ds(24 * p, 24), :] = (
                (acc3[par, p, pos[(p + 2) % 3]] + r3[par, p, 0]) + (r3[par, p, 1] + r3[par, p, 2]))

    def when_unit(v, step):
        pl.when(jnp.logical_and(v >= 0, v < UNITS))(lambda: step(v))

    def body(u, carry):
        li, task = u // NT, lax.rem(u, NT)
        slot = lax.rem(li, 2)
        par, g3 = lax.rem(u, 2), lax.rem(u, 3)
        computing = u < UNITS

        def dest(rel):
            if rel == 0:
                return gown.at[g3].reshape(64 * 72, 128)
            return gsend.at[par].reshape(64 * 72, 128)

        for k in range(NL):
            @pl.when(jnp.logical_and(task == 0, li == k))
            def _(k=k):
                for cp in loads(NL - 1 - k, k % 2):
                    cp.wait()
                if k + 1 < NL:
                    for cp in loads(NL - 2 - k, (k + 1) % 2):
                        cp.start()

        @pl.when(computing)
        def _():
            for m in range(4):
                val = jnp.dot(at[slot, 384 * m:384 * (m + 1), :], dbuf[task], preferred_element_type=F32)
                for lb in range(3):
                    tmp[m % 2, lb] = val[:, 128 * lb:128 * (lb + 1)]
                for rel in range(2):
                    cc = core if rel == 0 else 1 - core
                    dst = dest(rel)
                    for j in range(12):
                        for lb in range(3):
                            dst[pl.ds(m * 16 * 72 + 36 + 3 * j + lb, 16, stride=72), :] = (
                                tmp[m % 2, lb, pl.ds(12 * cc + j, 16, stride=24), :])

        when_unit(u - 3, step_relay2)
        when_unit(u - 4, step_last3)

        @pl.when(computing)
        def _():
            def block(mb, c):
                rows = pl.ds(pl.multiple_of(mb * 512, 512), 512)
                for n in range(6):
                    cols = slice(256 * n, 256 * (n + 1))
                    val = jnp.dot(dbuf[task, rows, :], w2t[slot, :, cols], preferred_element_type=F32)
                    sbuf[rows, cols] = (val * sl[slot, rows, cols]).astype(BF16)
                return c
            lax.fori_loop(0, 2, block, 0)

        when_unit(u - 1, step_d2d)

        @pl.when(computing)
        def _():
            for n in range(6):
                val = jnp.dot(ht[slot], sbuf[:, 256 * n:256 * (n + 1)], preferred_element_type=F32)
                for lb in range(2):
                    tmp[n % 2, lb] = val[:, 128 * lb:128 * (lb + 1)]
                for rel in range(2):
                    cc = core if rel == 0 else 1 - core
                    dst = dest(rel)
                    for r in range(3):
                        for lb in range(2):
                            dst[pl.ds(12 * r + 2 * n + lb, 64, stride=72), :] = (
                                tmp[n % 2, lb, pl.ds(3 * cc + r, 64, stride=6), :])

        when_unit(u, lambda v: start(d2d_copies(v)))
        when_unit(u - 3, step_main2)
        when_unit(u - 2, step_main1)

        @pl.when(u < UNITS - NT)
        def _():
            def block(mb, c):
                rows = pl.ds(pl.multiple_of(mb * 512, 512), 512)
                val = jnp.dot(sbuf[rows, :], w1t[slot], preferred_element_type=F32)
                dbuf[task, rows, :] = (dbuf[task, rows, :].astype(F32) + val).astype(BF16)
                return c
            lax.fori_loop(0, 2, block, 0)

        when_unit(u - 1, step_relay1)
        return carry

    lax.fori_loop(0, UNITS + 4, body, 0)


def backward(acts_t, hid_t, slopes, w1t, w2t, d0):
    any_spec = pl.BlockSpec(memory_space=pl.ANY)
    dma = pltpu.SemaphoreType.DMA
    scratch = [
        pltpu.VMEM((2, DF, TOK), BF16),
        pltpu.VMEM((2, DM, TOK), BF16),
        pltpu.VMEM((2, TOK, DF), F32),
        pltpu.VMEM((2, DF, DM), BF16),
        pltpu.VMEM((2, DM, DF), BF16),
        pltpu.VMEM((NT, TOK, DM), BF16),
        pltpu.VMEM((TOK, DF), BF16),
        pltpu.VMEM((2, 3, 384, 128), F32),
        pltpu.VMEM((3, 4, 4, 4, 72, 128), F32),
        pltpu.VMEM((2, 4, 4, 4, 72, 128), F32),
        pltpu.VMEM((2, 4, 4, 4, 72, 128), F32),
        pltpu.VMEM((2, 3, 2, 2, 4, 24, 128), F32),
        pltpu.VMEM((2, 3, 2, 4, 4, 24, 128), F32),
        pltpu.VMEM((2, 3, 4, 4, 24, 128), F32),
        pltpu.VMEM((2, 3, 2, 2, 24, 128), F32),
        pltpu.VMEM((2, 3, 2, 4, 24, 128), F32),
        pltpu.VMEM((2, 3, 4, 24, 128), F32),
        pltpu.VMEM((2, 3, 3, 24, 128), F32),
        dma((5, 2)), dma, dma((2,)), dma((2,)),
        dma((2, 3, 2)), dma((2, 3, 2)), dma((2, 3, 2)), dma((2, 3, 2)),
        dma((2, 3, 2)), dma((2, 3, 2)), dma((2, 3, 2)), dma((2, 3, 2)),
        dma((2, 3, 3)), dma((2, 3, 3)),
    ]
    return pl.pallas_call(
        backward_kernel,
        out_shape=jax.ShapeDtypeStruct((UNITS, 72, 128), F32),
        in_specs=[any_spec] * 15,
        out_specs=pl.BlockSpec(memory_space=pltpu.VMEM),
        scratch_shapes=scratch,
        compiler_params=pltpu.CompilerParams(
            collective_id=0, has_side_effects=True, vmem_limit_bytes=67043328),
        cost_estimate=pl.CostEstimate(flops=58 * 10**9, bytes_accessed=60 * 10**6, transcendentals=0),
    )(*acts_t, *hid_t, *slopes, w1t, w2t, d0)


def solution(mesh):
    num_dev = mesh.shape['data']

    def local_step(x_local, lab_local, w_up, w_down, task_heads):
        num_layers = w_up.shape[0]
        num_classes = task_heads.shape[2]
        inv_tokens = 1.0 / (x_local.shape[0] * num_dev)
        hidden = x_local
        acts_t, hid_t, slopes = [], [], []
        for layer_idx in range(num_layers):
            pre_act = jnp.dot(hidden, w_up[layer_idx], preferred_element_type=F32)
            act_val, gelu_slope = jax.jvp(jax.nn.gelu, (pre_act,), (jnp.ones_like(pre_act),))
            act_bf = act_val.astype(BF16)
            mlp_out = jnp.dot(act_bf, w_down[layer_idx], preferred_element_type=F32)
            acts_t.append(act_bf.T)
            hid_t.append(hidden.T)
            slopes.append(gelu_slope)
            hidden = (hidden.astype(F32) + mlp_out).astype(BF16)
        logits = jnp.einsum('bd,tdc->tbc', hidden, task_heads, preferred_element_type=F32)
        soft_probs = jax.nn.softmax(logits, axis=-1)
        onehot = (lab_local[:, :, None] == jnp.arange(num_classes)[None, None, :]).astype(F32)
        head_err = (soft_probs - onehot).astype(BF16)
        d_hidden = jnp.einsum('tbc,tdc->tbd', head_err, task_heads, preferred_element_type=F32).astype(BF16)
        shares = backward(acts_t, hid_t, slopes, jnp.swapaxes(w_up, 1, 2), jnp.swapaxes(w_down, 1, 2), d_hidden)
        shares = shares.reshape(num_layers, NT, 72 * 128)[::-1] * inv_tokens
        gram_part = jnp.sum(shares[:, :, None, :] * shares[:, None, :, :], axis=(0, 3))
        gram_mat = lax.psum(gram_part, 'data')
        task_weights = simplex_weights(gram_mat)
        mixed = jnp.sum(task_weights[None, :, None] * shares, axis=1)
        return task_weights, gram_mat, mixed[:, :36 * 128], mixed[:, 36 * 128:]

    return jax.shard_map(local_step, mesh=mesh, in_specs=(P('data', None), P(None, 'data'), P(), P(), P()), out_specs=(P(), P(), P(None, 'data'), P(None, 'data')), check_vma=False)
```

```python
import jax
import jax.numpy as jnp
from jax import lax
from jax.experimental import pallas as pl
from jax.experimental.pallas import tpu as pltpu
from jax.sharding import PartitionSpec as P

EG_STEPS = 20
NT = 3
NL = 4
DM = 384
DF = 1536
TOK = 1024
NC = 13
LN = 128
ROWS = 72
HALF = 36
GRP = 24
BLK = 256
GRID = (4, 4, 4)
GELU_C = 0.7978845608028654
GELU_K = 0.044715
UNITS = NT * NL
AXIS_STRIDE = (2, 8, 32)
MESH = pl.DeviceIdType.MESH
F32 = jnp.float32
BF16 = jnp.bfloat16


def half_slice(half):
    return slice(None) if half is None else pl.ds(2 * half, 2)


def step_kernel(x_hbm, lab_ref, w1_hbm, w2_hbm, heads_ref,
                alpha_ref, gram_ref, up_ref, down_ref, at_save, ht_save, sl_save,
                at, ht, sl, w1, w2, hbuf, dbuf, sbuf, ident, tmp,
                gown, gsend, rd2d, ra1, rb1, acc2, ra2, rb2, acc3, r3, res, mix, gcore, gax,
                x_sem, w_sem, save_sem, load_sem, d2d_s, d2d_r, a1_s, a1_r, b1_s, b1_r,
                a2_s, a2_r, b2_s, b2_r, c3_s, c3_r, gc_s, gc_r, gx_s, gx_r):
    me = lax.axis_index('data')
    core = lax.rem(me, 2)
    pos = [lax.rem(me // s, 4) for s in AXIS_STRIDE]
    sibling = me + 1 - 2 * core

    def at_pos(axis, k):
        return lax.rem(pos[axis] + k, 4)

    def peer(axis, k):
        return me + (at_pos(axis, k) - pos[axis]) * AXIS_STRIDE[axis]

    barrier = pltpu.get_barrier_semaphore()
    partners = [sibling] + [peer(a, k) for a in range(3) for k in (1, 2, 3)]
    for dev in partners:
        pl.semaphore_signal(barrier, inc=1, device_id=(dev,), device_id_type=MESH)

    def w_loads(layer, slot):
        return [pltpu.make_async_copy(w1_hbm.at[layer], w1.at[slot], w_sem.at[0, slot]),
                pltpu.make_async_copy(w2_hbm.at[layer], w2.at[slot], w_sem.at[1, slot])]

    def saves(layer):
        return [pltpu.make_async_copy(at.at[layer], at_save.at[layer], save_sem.at[0, layer]),
                pltpu.make_async_copy(ht.at[layer], ht_save.at[layer], save_sem.at[1, layer]),
                pltpu.make_async_copy(sl.at[layer], sl_save.at[layer], save_sem.at[2, layer])]

    def loads(layer):
        return [pltpu.make_async_copy(at_save.at[layer], at.at[layer], load_sem.at[0, layer]),
                pltpu.make_async_copy(ht_save.at[layer], ht.at[layer], load_sem.at[1, layer]),
                pltpu.make_async_copy(sl_save.at[layer], sl.at[layer], load_sem.at[2, layer])] + w_loads(layer, layer)

    x_load = pltpu.make_async_copy(x_hbm, hbuf, x_sem)
    x_load.start()
    for cp in w_loads(0, 0):
        cp.start()
    ident[...] = (lax.broadcasted_iota(jnp.int32, (256, 256), 0)
                  == lax.broadcasted_iota(jnp.int32, (256, 256), 1)).astype(F32).astype(BF16)
    x_load.wait()

    def nt_dot(a, b):
        return lax.dot_general(a, b, (((1,), (1,)), ((), ())), preferred_element_type=F32)

    def forward(layer, carry):
        slot = lax.rem(layer, 2)
        for cp in w_loads(layer, slot):
            cp.wait()

        @pl.when(layer < NL - 1)
        def _():
            for cp in w_loads(layer + 1, 1 - slot):
                cp.start()

        @pl.when(layer >= 2)
        def _():
            for cp in saves(layer - 2):
                cp.wait()

        for n in range(3):
            ht[slot, LN * n:LN * (n + 1), :] = nt_dot(
                ident[0:128, 0:128], hbuf[:, LN * n:LN * (n + 1)]).astype(BF16)

        def up(mb, c):
            rows = pl.ds(pl.multiple_of(mb * 256, 256), 256)
            for n in range(6):
                cols = slice(BLK * n, BLK * (n + 1))
                x = jnp.dot(hbuf[rows, :], w1[slot, :, cols], preferred_element_type=F32)
                x2 = x * x
                th = jnp.tanh(x * (GELU_C + (GELU_C * GELU_K) * x2))
                hp = 0.5 + 0.5 * th
                act = x * hp
                sbuf[rows, cols] = act.astype(BF16)
                sl[slot, rows, cols] = hp + act * ((1.0 - th) * (GELU_C + (3.0 * GELU_C * GELU_K) * x2))
            return c

        lax.fori_loop(0, 4, up, 0)
        for n in range(6):
            cols = slice(BLK * n, BLK * (n + 1))
            at[slot, cols, :] = nt_dot(ident[...], sbuf[:, cols]).astype(BF16)

        @pl.when(layer < 2)
        def _():
            for cp in saves(layer):
                cp.start()

        def down(mb, c):
            rows = pl.ds(pl.multiple_of(mb * 512, 512), 512)
            val = jnp.dot(sbuf[rows, :], w2[slot], preferred_element_type=F32)
            hbuf[rows, :] = (hbuf[rows, :].astype(F32) + val).astype(BF16)
            return c

        lax.fori_loop(0, 2, down, 0)
        return carry

    lax.fori_loop(0, NL, forward, 0)

    logits = nt_dot(heads_ref[...], hbuf[...])
    class_id = lax.broadcasted_iota(jnp.int32, (16, TOK), 0)
    for t in range(NT):
        lg = jnp.where(class_id < NC, logits[16 * t:16 * (t + 1), :], -jnp.inf)
        ex = jnp.exp(lg - jnp.max(lg, axis=0, keepdims=True))
        prob = ex / jnp.sum(ex, axis=0, keepdims=True)
        onehot = (class_id == lab_ref[t:t + 1, :]).astype(F32)
        err = jnp.transpose(prob - onehot).astype(BF16)
        dbuf[t] = jnp.dot(err, heads_ref[16 * t:16 * (t + 1), :], preferred_element_type=F32).astype(BF16)

    pl.semaphore_wait(barrier, len(partners))

    def remote(src, dst, send, recv, dev):
        return pltpu.make_async_remote_copy(
            src_ref=src, dst_ref=dst, send_sem=send, recv_sem=recv,
            device_id=(dev,), device_id_type=MESH)

    def chunk1(g3, p, idx, half=None):
        h, rows = half_slice(half), pl.ds(24 * p, 24)
        return (gown.at[g3, h, :, idx, rows, :], gown.at[g3, h, idx, :, rows, :],
                gown.at[g3, idx, h, :, rows, :])[p]

    def chunk2(par, p, idx, half=None):
        h = half_slice(half)
        return (acc2.at[par, 0, h, idx], acc2.at[par, 1, idx, h], acc2.at[par, 2, h, idx])[p]

    def d2d_copies(v):
        par = lax.rem(v, 2)
        return [remote(gsend.at[par], rd2d.at[par], d2d_s.at[par], d2d_r.at[par], sibling)]

    def relay1(v):
        par, g3 = lax.rem(v, 2), lax.rem(v, 3)
        return [remote(chunk1(g3, p, at_pos(p, 2), d), ra1.at[par, p, d], a1_s.at[par, p, d],
                       a1_r.at[par, p, d], peer(p, 1 + 2 * d)) for p in range(3) for d in range(2)]

    def main1(v):
        par, g3 = lax.rem(v, 2), lax.rem(v, 3)
        return [remote(chunk1(g3, p, at_pos(p, 1 + 2 * d)), rb1.at[par, p, d], b1_s.at[par, p, d],
                       b1_r.at[par, p, d], peer(p, 1 + 2 * d)) for p in range(3) for d in range(2)]

    def relay2(v):
        par = lax.rem(v, 2)
        return [remote(chunk2(par, p, at_pos((p + 1) % 3, 2), d), ra2.at[par, p, d], a2_s.at[par, p, d],
                       a2_r.at[par, p, d], peer((p + 1) % 3, 1 + 2 * d)) for p in range(3) for d in range(2)]

    def main2(v):
        par = lax.rem(v, 2)
        return [remote(chunk2(par, p, at_pos((p + 1) % 3, 1 + 2 * d)), rb2.at[par, p, d], b2_s.at[par, p, d],
                       b2_r.at[par, p, d], peer((p + 1) % 3, 1 + 2 * d)) for p in range(3) for d in range(2)]

    def last3(v):
        par = lax.rem(v, 2)
        return [remote(acc3.at[par, p, at_pos((p + 2) % 3, k)], r3.at[par, p, k - 1], c3_s.at[par, p, k - 1],
                       c3_r.at[par, p, k - 1], peer((p + 2) % 3, k)) for p in range(3) for k in (1, 2, 3)]

    def start(copies):
        for cp in copies:
            cp.start()

    def wait(copies):
        for cp in copies:
            cp.wait()

    def step_d2d(v):
        wait(d2d_copies(v))
        par, g3 = lax.rem(v, 2), lax.rem(v, 3)

        def add(i, carry):
            gown[g3, i] = gown[g3, i] + rd2d[par, i]
            return carry

        lax.fori_loop(0, 4, add, 0)
        start(relay1(v))

    def step_relay1(v):
        wait(relay1(v))
        par, g3 = lax.rem(v, 2), lax.rem(v, 3)
        for p in range(3):
            for d in range(2):
                dst = chunk1(g3, p, at_pos(p, 1 + 2 * d), d)
                dst[...] = dst[...] + ra1[par, p, d]
        start(main1(v))

    def step_main1(v):
        wait(main1(v))
        par, g3 = lax.rem(v, 2), lax.rem(v, 3)
        for p in range(3):
            acc2[par, p] = chunk1(g3, p, pos[p])[...] + rb1[par, p, 0] + rb1[par, p, 1]
        start(relay2(v))

    def step_relay2(v):
        wait(relay2(v))
        par = lax.rem(v, 2)
        for p in range(3):
            for d in range(2):
                dst = chunk2(par, p, at_pos((p + 1) % 3, 1 + 2 * d), d)
                dst[...] = dst[...] + ra2[par, p, d]
        start(main2(v))

    def step_main2(v):
        wait(main2(v))
        par = lax.rem(v, 2)
        for p in range(3):
            acc3[par, p] = chunk2(par, p, pos[(p + 1) % 3])[...] + rb2[par, p, 0] + rb2[par, p, 1]
        start(last3(v))

    def step_last3(v):
        wait(last3(v))
        par = lax.rem(v, 2)
        for p in range(3):
            res[v, pl.ds(24 * p, 24), :] = (
                (acc3[par, p, pos[(p + 2) % 3]] + r3[par, p, 0]) + (r3[par, p, 1] + r3[par, p, 2]))

    def when_unit(v, step):
        pl.when(jnp.logical_and(v >= 0, v < UNITS))(lambda: step(v))

    def body(u, carry):
        li, task = u // NT, lax.rem(u, NT)
        slot = lax.rem(li + 1, 2)
        par, g3 = lax.rem(u, 2), lax.rem(u, 3)
        computing = u < UNITS

        def dest(rel):
            if rel == 0:
                return gown.at[g3].reshape(64 * ROWS, LN)
            return gsend.at[par].reshape(64 * ROWS, LN)

        for k in (2, 3):
            @pl.when(u == NT * (k - 1))
            def _(k=k):
                for cp in loads(NL - 1 - k):
                    cp.start()

            @pl.when(u == NT * k)
            def _(k=k):
                for cp in loads(NL - 1 - k):
                    cp.wait()

        @pl.when(computing)
        def _():
            for m in range(4):
                val = jnp.dot(at[slot, 384 * m:384 * (m + 1), :], dbuf[task], preferred_element_type=F32)
                for lb in range(3):
                    tmp[m % 2, lb] = val[:, LN * lb:LN * (lb + 1)]
                for rel in range(2):
                    cc = core if rel == 0 else 1 - core
                    dst = dest(rel)
                    for j in range(12):
                        for lb in range(3):
                            dst[pl.ds(m * 16 * 72 + 36 + 3 * j + lb, 16, stride=ROWS), :] = (
                                tmp[m % 2, lb, pl.ds(12 * cc + j, 16, stride=24), :])

        when_unit(u - 3, step_relay2)
        when_unit(u - 4, step_last3)

        @pl.when(computing)
        def _():
            def block(mb, c):
                rows = pl.ds(pl.multiple_of(mb * 512, 512), 512)
                for n in range(6):
                    cols = slice(BLK * n, BLK * (n + 1))
                    val = nt_dot(dbuf[task, rows, :], w2[slot, cols, :])
                    sbuf[rows, cols] = (val * sl[slot, rows, cols]).astype(BF16)
                return c
            lax.fori_loop(0, 2, block, 0)

        when_unit(u - 1, step_d2d)

        @pl.when(computing)
        def _():
            for n in range(6):
                val = jnp.dot(ht[slot], sbuf[:, BLK * n:BLK * (n + 1)], preferred_element_type=F32)
                for lb in range(2):
                    tmp[n % 2, lb] = val[:, LN * lb:LN * (lb + 1)]
                for rel in range(2):
                    cc = core if rel == 0 else 1 - core
                    dst = dest(rel)
                    for r in range(3):
                        for lb in range(2):
                            dst[pl.ds(12 * r + 2 * n + lb, 64, stride=ROWS), :] = (
                                tmp[n % 2, lb, pl.ds(3 * cc + r, 64, stride=6), :])

        when_unit(u, lambda v: start(d2d_copies(v)))
        when_unit(u - 3, step_main2)
        when_unit(u - 2, step_main1)

        @pl.when(u < UNITS - NT)
        def _():
            def block(mb, c):
                rows = pl.ds(pl.multiple_of(mb * 512, 512), 512)
                val = nt_dot(sbuf[rows, :], w1[slot])
                dbuf[task, rows, :] = (dbuf[task, rows, :].astype(F32) + val).astype(BF16)
                return c
            lax.fori_loop(0, 2, block, 0)

        when_unit(u - 1, step_relay1)
        return carry

    lax.fori_loop(0, UNITS + 4, body, 0)

    inv_tokens = 1.0 / (TOK * lax.axis_size('data'))
    pairs = [(t, s) for t in range(NT) for s in range(t, NT)]
    rows6 = []
    for t, s in pairs:
        prod = res[t] * res[s]
        for li in range(1, NL):
            prod = prod + res[NT * li + t] * res[NT * li + s]
        rows6.append(jnp.sum(prod, axis=0, keepdims=True))
    tile = jnp.concatenate(rows6 + [jnp.zeros((2, 128), F32)], axis=0) * (inv_tokens * inv_tokens)

    gcore[core] = tile
    cp = remote(gcore.at[core], gcore.at[core], gc_s, gc_r, sibling)
    cp.start()
    cp.wait()
    tile = gcore[0] + gcore[1]
    for a in range(3):
        gax[a, pos[a]] = tile
        copies = [remote(gax.at[a, pos[a]], gax.at[a, pos[a]], gx_s.at[a, k - 1], gx_r.at[a, k - 1], peer(a, k))
                  for k in (1, 2, 3)]
        start(copies)
        wait(copies)
        tile = (gax[a, 0] + gax[a, 1]) + (gax[a, 2] + gax[a, 3])

    sums = jnp.broadcast_to(jnp.sum(tile, axis=1, keepdims=True), (8, LN))
    gram = {}
    for i, (t, s) in enumerate(pairs):
        gram[t, s] = gram[s, t] = jnp.broadcast_to(sums[i:i + 1, :], (8, LN))
    temperature = (gram[0, 0] + gram[1, 1] + gram[2, 2]) / NT
    alpha = [jnp.full((8, LN), 1.0 / NT, F32)] * NT

    def eg_step(i, alpha):
        pull = [gram[t, 0] * alpha[0] + gram[t, 1] * alpha[1] + gram[t, 2] * alpha[2] for t in range(NT)]
        new = [alpha[t] * jnp.exp(-pull[t] / temperature) for t in range(NT)]
        total = new[0] + new[1] + new[2]
        return tuple(a / total for a in new)

    alpha = lax.fori_loop(0, EG_STEPS, eg_step, tuple(alpha))
    for t in range(NT):
        alpha_ref[t] = alpha[t][0, 0]
        for s in range(NT):
            gram_ref[t, s] = gram[t, s][0, 0]
    scale = [jnp.broadcast_to(alpha[t][0:1, :] * inv_tokens, (72, 128)) for t in range(NT)]
    for layer in range(NL):
        u = NT * (NL - 1 - layer)
        mix[72 * layer:72 * (layer + 1), :] = scale[0] * res[u] + scale[1] * res[u + 1] + scale[2] * res[u + 2]
    for k in range(36):
        up_ref[:, LN * k:LN * (k + 1)] = mix[pl.ds(k, NL, stride=ROWS), :]
        down_ref[:, LN * k:LN * (k + 1)] = mix[pl.ds(36 + k, NL, stride=ROWS), :]


def whole_step(x, labels, w_up, w_down, heads_t):
    any_spec = pl.BlockSpec(memory_space=pl.ANY)
    vmem_spec = pl.BlockSpec(memory_space=pltpu.VMEM)
    smem_spec = pl.BlockSpec(memory_space=pltpu.SMEM)
    dma = pltpu.SemaphoreType.DMA
    two, three = (2,), (3,)

    def vmem(*shape, dtype=F32):
        return pltpu.VMEM(shape, dtype)

    both = pltpu.SemaphoreType.DMA(two + three + two)
    triple = dma(three + three)
    scratch = [
        vmem(2, DF, TOK, dtype=BF16),
        vmem(2, DM, TOK, dtype=BF16),
        vmem(2, TOK, DF),
        vmem(2, DM, DF, dtype=BF16),
        vmem(2, DF, DM, dtype=BF16),
        vmem(TOK, DM, dtype=BF16),
        vmem(NT, TOK, DM, dtype=BF16),
        vmem(TOK, DF, dtype=BF16),
        vmem(BLK, BLK, dtype=BF16),
        vmem(2, 3, DM, LN),
        vmem(3, *GRID, ROWS, LN),
        vmem(2, *GRID, ROWS, LN),
        vmem(2, *GRID, ROWS, LN),
        vmem(2, 3, 2, 2, 4, GRP, LN),
        vmem(2, 3, 2, 4, 4, GRP, LN),
        vmem(2, 3, 4, 4, GRP, LN),
        vmem(2, 3, 2, 2, GRP, LN),
        vmem(2, 3, 2, 4, GRP, LN),
        vmem(2, 3, 4, GRP, LN),
        vmem(2, 3, 3, GRP, LN),
        vmem(UNITS, ROWS, LN),
        vmem(NL * ROWS, LN),
        vmem(2, 8, LN),
        vmem(3, 4, 8, LN),
        dma, dma(two + two), dma(three + two), dma(three + two), dma(two), dma(two),
        both, both, both, both, both, both, both, both,
        dma(two + three + three), dma(two + three + three), dma, dma, triple, triple,
    ]
    return pl.pallas_call(
        step_kernel,
        out_shape=(
            jax.ShapeDtypeStruct((NT,), F32),
            jax.ShapeDtypeStruct((NT, NT), F32),
            jax.ShapeDtypeStruct((NL, HALF * LN), F32),
            jax.ShapeDtypeStruct((NL, HALF * LN), F32),
            jax.ShapeDtypeStruct((2, DF, TOK), BF16),
            jax.ShapeDtypeStruct((2, DM, TOK), BF16),
            jax.ShapeDtypeStruct((2, TOK, DF), F32),
        ),
        in_specs=[any_spec, vmem_spec, any_spec, any_spec, vmem_spec],
        out_specs=(smem_spec, smem_spec, vmem_spec, vmem_spec, any_spec, any_spec, any_spec),
        scratch_shapes=scratch,
        compiler_params=pltpu.CompilerParams(
            collective_id=0, has_side_effects=True, vmem_limit_bytes=67043328),
    )(x, labels, w_up, w_down, heads_t)[:4]


def solution(mesh):
    def local_step(x_local, lab_local, w_up, w_down, task_heads):
        heads_t = jnp.pad(jnp.swapaxes(task_heads, 1, 2), ((0, 0), (0, 16 - NC), (0, 0))).reshape(NT * 16, DM)
        return whole_step(x_local, lab_local, w_up, w_down, heads_t)

    return jax.shard_map(local_step, mesh=mesh, in_specs=(P('data', None), P(None, 'data'), P(), P(), P()), out_specs=(P(), P(), P(None, 'data'), P(None, 'data')), check_vma=False)
```

```python
import jax
import jax.numpy as jnp
from jax import lax
from jax.experimental import pallas as pl
from jax.experimental.pallas import tpu as pltpu
from jax.sharding import PartitionSpec as P

EG_STEPS = 20
NT = 3
NL = 4
DM = 384
DF = 1536
TOK = 1024
NC = 13
LN = 128
ROWS = 72
HALF = 36
GRP = 24
BLK = 256
GRID = (4, 4, 4)
GELU_C = 0.7978845608028654
GELU_K = 0.044715
UNITS = NT * NL
DUE = (5, 8, 11, 14, 17, 20)
AXIS_STRIDE = (2, 8, 32)
MESH = pl.DeviceIdType.MESH
F32 = jnp.float32
BF16 = jnp.bfloat16


def half_slice(half):
    return slice(None) if half is None else pl.ds(2 * half, 2)


def step_kernel(x_hbm, lab_ref, w1_hbm, w2_hbm, heads_ref,
                alpha_ref, gram_ref, up_ref, down_ref, at_save, ht_save, sl_save,
                at, ht, sl, w1, w2, hbuf, dbuf, sbuf, ident, tmp,
                gown, gsend, rd2d, ra1, rb1, acc2, ra2, rb2, acc3, r3, res, mix, gcore, gax,
                x_sem, w_sem, save_sem, load_sem, d2d_s, d2d_r, a1_s, a1_r, b1_s, b1_r,
                a2_s, a2_r, b2_s, b2_r, c3_s, c3_r, e1_s, e1_r, e2_s, e2_r, gc_s, gc_r, gx_s, gx_r):
    me = lax.axis_index('data')
    core = lax.rem(me, 2)
    pos = [lax.rem(me // s, 4) for s in AXIS_STRIDE]
    sibling = me + 1 - 2 * core

    def at_pos(axis, k):
        return lax.rem(pos[axis] + k, 4)

    def peer(axis, k):
        return me + (at_pos(axis, k) - pos[axis]) * AXIS_STRIDE[axis]

    barrier = pltpu.get_barrier_semaphore()
    row_peers = [sibling] + [dev + c * (sibling - me) for dev in (peer(0, 1), peer(0, 2), peer(0, 3)) for c in range(2)]
    plane_peers = [me + peer(1, j) - me + peer(2, k) - me for k in range(4) for j in range(4) if j + k]
    partners = row_peers + plane_peers
    for dev in partners:
        pl.semaphore_signal(barrier, inc=1, device_id=(dev,), device_id_type=MESH)

    def w_loads(layer, slot):
        return [pltpu.make_async_copy(w1_hbm.at[layer], w1.at[slot], w_sem.at[0, slot]),
                pltpu.make_async_copy(w2_hbm.at[layer], w2.at[slot], w_sem.at[1, slot])]

    def saves(layer):
        return [pltpu.make_async_copy(at.at[layer], at_save.at[layer], save_sem.at[0, layer]),
                pltpu.make_async_copy(ht.at[layer], ht_save.at[layer], save_sem.at[1, layer]),
                pltpu.make_async_copy(sl.at[layer], sl_save.at[layer], save_sem.at[2, layer])]

    def loads(layer):
        return [pltpu.make_async_copy(at_save.at[layer], at.at[layer], load_sem.at[0, layer]),
                pltpu.make_async_copy(ht_save.at[layer], ht.at[layer], load_sem.at[1, layer]),
                pltpu.make_async_copy(sl_save.at[layer], sl.at[layer], load_sem.at[2, layer])] + w_loads(layer, layer)

    x_load = pltpu.make_async_copy(x_hbm, hbuf, x_sem)
    x_load.start()
    for cp in w_loads(0, 0):
        cp.start()
    ident[...] = (lax.broadcasted_iota(jnp.int32, (256, 256), 0)
                  == lax.broadcasted_iota(jnp.int32, (256, 256), 1)).astype(F32).astype(BF16)
    x_load.wait()

    def nt_dot(a, b):
        return lax.dot_general(a, b, (((1,), (1,)), ((), ())), preferred_element_type=F32)

    def forward(layer, carry):
        slot = lax.rem(layer, 2)
        for cp in w_loads(layer, slot):
            cp.wait()

        @pl.when(layer < NL - 1)
        def _():
            for cp in w_loads(layer + 1, 1 - slot):
                cp.start()

        @pl.when(layer >= 2)
        def _():
            for cp in saves(layer - 2):
                cp.wait()

        for n in range(3):
            ht[slot, LN * n:LN * (n + 1), :] = nt_dot(
                ident[0:128, 0:128], hbuf[:, LN * n:LN * (n + 1)]).astype(BF16)

        def up(mb, c):
            rows = slice(None)
            for n in range(6):
                cols = slice(BLK * n, BLK * (n + 1))
                x = jnp.dot(hbuf[rows, :], w1[slot, :, cols], preferred_element_type=F32)
                x2 = x * x
                th = jnp.tanh(x * (GELU_C + (GELU_C * GELU_K) * x2))
                hp = 0.5 + 0.5 * th
                act = x * hp
                sbuf[rows, cols] = act.astype(BF16)
                sl[slot, rows, cols] = hp + act * ((1.0 - th) * (GELU_C + (3.0 * GELU_C * GELU_K) * x2))
            return c

        up(0, 0)
        for n in range(6):
            cols = slice(BLK * n, BLK * (n + 1))
            at[slot, cols, :] = nt_dot(ident[...], sbuf[:, cols]).astype(BF16)

        @pl.when(layer < 2)
        def _():
            for cp in saves(layer):
                cp.start()

        def down(mb, c):
            rows = slice(None)
            val = jnp.dot(sbuf[rows, :], w2[slot], preferred_element_type=F32)
            hbuf[rows, :] = (hbuf[rows, :].astype(F32) + val).astype(BF16)
            return c

        down(0, 0)
        return carry

    lax.fori_loop(0, NL, forward, 0)

    logits = nt_dot(heads_ref[...], hbuf[...])
    class_id = lax.broadcasted_iota(jnp.int32, (16, TOK), 0)
    for t in range(NT):
        lg = jnp.where(class_id < NC, logits[16 * t:16 * (t + 1), :], -jnp.inf)
        ex = jnp.exp(lg - jnp.max(lg, axis=0, keepdims=True))
        prob = ex / jnp.sum(ex, axis=0, keepdims=True)
        onehot = (class_id == lab_ref[t:t + 1, :]).astype(F32)
        err = jnp.transpose(prob - onehot).astype(BF16)
        dbuf[t] = jnp.dot(err, heads_ref[16 * t:16 * (t + 1), :], preferred_element_type=F32).astype(BF16)

    pl.semaphore_wait(barrier, len(partners))

    def remote(src, dst, send, recv, dev):
        return pltpu.make_async_remote_copy(
            src_ref=src, dst_ref=dst, send_sem=send, recv_sem=recv,
            device_id=(dev,), device_id_type=MESH)

    def chunk1(g3, p, idx, half=None):
        h, rows = half_slice(half), pl.ds(24 * p, 24)
        return (gown.at[g3, h, :, idx, rows, :], gown.at[g3, h, idx, :, rows, :],
                gown.at[g3, idx, h, :, rows, :])[p]

    def chunk2(par, p, idx, half=None):
        h = half_slice(half)
        return (acc2.at[par, 0, h, idx], acc2.at[par, 1, idx, h], acc2.at[par, 2, h, idx])[p]

    def d2d_copies(v):
        par = lax.rem(v, 2)
        return [remote(gsend.at[par], rd2d.at[par], d2d_s.at[par], d2d_r.at[par], sibling)]

    def relay1(v):
        par = g3 = lax.rem(v, 3)
        return [remote(chunk1(g3, p, at_pos(p, 2), d), ra1.at[par, p, d], a1_s.at[par, p, d],
                       a1_r.at[par, p, d], peer(p, 1 + 2 * d)) for p in range(3) for d in range(2)]

    def direct1(v):
        par = g3 = lax.rem(v, 3)
        return [remote(chunk1(g3, p, at_pos(p, 1 + 2 * d), 1 - d), rb1.at[par, p, d, half_slice(1 - d)],
                       e1_s.at[par, p, d], e1_r.at[par, p, d], peer(p, 1 + 2 * d)) for p in range(3) for d in range(2)]

    def main1(v):
        par = g3 = lax.rem(v, 3)
        return [remote(chunk1(g3, p, at_pos(p, 1 + 2 * d), d), rb1.at[par, p, d, half_slice(d)], b1_s.at[par, p, d],
                       b1_r.at[par, p, d], peer(p, 1 + 2 * d)) for p in range(3) for d in range(2)]

    def relay2(v):
        par = lax.rem(v, 3)
        return [remote(chunk2(par, p, at_pos((p + 1) % 3, 2), d), ra2.at[par, p, d], a2_s.at[par, p, d],
                       a2_r.at[par, p, d], peer((p + 1) % 3, 1 + 2 * d)) for p in range(3) for d in range(2)]

    def direct2(v):
        par = lax.rem(v, 3)
        return [remote(chunk2(par, p, at_pos((p + 1) % 3, 1 + 2 * d), 1 - d), rb2.at[par, p, d, half_slice(1 - d)],
                       e2_s.at[par, p, d], e2_r.at[par, p, d], peer((p + 1) % 3, 1 + 2 * d))
                for p in range(3) for d in range(2)]

    def main2(v):
        par = lax.rem(v, 3)
        return [remote(chunk2(par, p, at_pos((p + 1) % 3, 1 + 2 * d), d), rb2.at[par, p, d, half_slice(d)],
                       b2_s.at[par, p, d], b2_r.at[par, p, d], peer((p + 1) % 3, 1 + 2 * d))
                for p in range(3) for d in range(2)]

    def last3(v):
        par = lax.rem(v, 3)
        return [remote(acc3.at[par, p, at_pos((p + 2) % 3, k)], r3.at[par, p, k - 1], c3_s.at[par, p, k - 1],
                       c3_r.at[par, p, k - 1], peer((p + 2) % 3, k)) for p in range(3) for k in (1, 2, 3)]

    def share(peers, slot, send, recv):
        copies = [remote(slot, slot, send.at[i], recv.at[i], dev) for i, dev in enumerate(peers)]
        for cp in copies:
            cp.start()
        for cp in copies:
            cp.wait()

    def tree_sum(terms):
        while len(terms) > 1:
            terms = [a + b for a, b in zip(terms[::2], terms[1::2])]
        return terms[0]

    def start(copies):
        for cp in copies:
            cp.start()

    def wait(copies):
        for cp in copies:
            cp.wait()

    def step_d2d(v):
        wait(d2d_copies(v))
        par, g3 = lax.rem(v, 2), lax.rem(v, 3)

        def add(i, carry):
            gown[g3, i] = gown[g3, i] + rd2d[par, i]
            return carry

        lax.fori_loop(0, 4, add, 0)
        start(relay1(v) + direct1(v))

    def step_relay1(v):
        wait(relay1(v))
        par = g3 = lax.rem(v, 3)
        for p in range(3):
            for d in range(2):
                dst = chunk1(g3, p, at_pos(p, 1 + 2 * d), d)
                dst[...] = dst[...] + ra1[par, p, d]
        start(main1(v))

    def step_main1(v):
        wait(main1(v) + direct1(v))
        par = g3 = lax.rem(v, 3)
        for p in range(3):
            acc2[par, p] = chunk1(g3, p, pos[p])[...] + rb1[par, p, 0] + rb1[par, p, 1]
        start(relay2(v) + direct2(v))

    def step_relay2(v):
        wait(relay2(v))
        par = lax.rem(v, 3)
        for p in range(3):
            for d in range(2):
                dst = chunk2(par, p, at_pos((p + 1) % 3, 1 + 2 * d), d)
                dst[...] = dst[...] + ra2[par, p, d]
        start(main2(v))

    def step_main2(v):
        wait(main2(v) + direct2(v))
        par = lax.rem(v, 3)
        for p in range(3):
            acc3[par, p] = chunk2(par, p, pos[(p + 1) % 3])[...] + rb2[par, p, 0] + rb2[par, p, 1]
        start(last3(v))

    def step_last3(v):
        wait(last3(v))
        par = lax.rem(v, 3)
        for p in range(3):
            res[v, pl.ds(24 * p, 24), :] = (
                (acc3[par, p, pos[(p + 2) % 3]] + r3[par, p, 0]) + (r3[par, p, 1] + r3[par, p, 2]))

    def when_unit(v, step):
        pl.when(jnp.logical_and(v >= 0, v < UNITS))(lambda: step(v))

    steps = (step_d2d, step_relay1, step_main1, step_relay2, step_main2, step_last3)

    def run_slot(u, k):
        for due, step in reversed(tuple(zip(DUE, steps))):
            if due % 4 == k:
                when_unit(u - due // 4, step)

    def body(u, carry):
        li, task = u // NT, lax.rem(u, NT)
        slot = lax.rem(li + 1, 2)
        par, g3 = lax.rem(u, 2), lax.rem(u, 3)
        computing = u < UNITS

        def dest(rel):
            if rel == 0:
                return gown.at[g3].reshape(64 * ROWS, LN)
            return gsend.at[par].reshape(64 * ROWS, LN)

        for k in (2, 3):
            @pl.when(u == NT * (k - 1))
            def _(k=k):
                for cp in loads(NL - 1 - k):
                    cp.start()

            @pl.when(u == NT * k)
            def _(k=k):
                for cp in loads(NL - 1 - k):
                    cp.wait()

        @pl.when(computing)
        def _():
            for m in range(4):
                val = jnp.dot(at[slot, 384 * m:384 * (m + 1), :], dbuf[task], preferred_element_type=F32)
                for lb in range(3):
                    tmp[m % 2, lb] = val[:, LN * lb:LN * (lb + 1)]
                for rel in range(2):
                    cc = core if rel == 0 else 1 - core
                    dst = dest(rel)
                    for j in range(12):
                        for lb in range(3):
                            dst[pl.ds(m * 16 * 72 + 36 + 3 * j + lb, 16, stride=ROWS), :] = (
                                tmp[m % 2, lb, pl.ds(12 * cc + j, 16, stride=24), :])

        run_slot(u, 0)

        @pl.when(computing)
        def _():
            def block(mb, c):
                rows = slice(None)
                for n in range(6):
                    cols = slice(BLK * n, BLK * (n + 1))
                    val = nt_dot(dbuf[task, rows, :], w2[slot, cols, :])
                    sbuf[rows, cols] = (val * sl[slot, rows, cols]).astype(BF16)
                return c
            block(0, 0)

        run_slot(u, 1)

        @pl.when(computing)
        def _():
            for n in range(6):
                val = jnp.dot(ht[slot], sbuf[:, BLK * n:BLK * (n + 1)], preferred_element_type=F32)
                for lb in range(2):
                    tmp[n % 2, lb] = val[:, LN * lb:LN * (lb + 1)]
                for rel in range(2):
                    cc = core if rel == 0 else 1 - core
                    dst = dest(rel)
                    for r in range(3):
                        for lb in range(2):
                            dst[pl.ds(12 * r + 2 * n + lb, 64, stride=ROWS), :] = (
                                tmp[n % 2, lb, pl.ds(3 * cc + r, 64, stride=6), :])

        when_unit(u, lambda v: start(d2d_copies(v)))
        run_slot(u, 2)

        @pl.when(u < UNITS - NT)
        def _():
            def block(mb, c):
                rows = slice(None)
                val = nt_dot(sbuf[rows, :], w1[slot])
                dbuf[task, rows, :] = (dbuf[task, rows, :].astype(F32) + val).astype(BF16)
                return c
            block(0, 0)

        run_slot(u, 3)
        return carry

    lax.fori_loop(0, UNITS + DUE[-1] // 4, body, 0)

    inv_tokens = 1.0 / (TOK * lax.axis_size('data'))
    pairs = [(t, s) for t in range(NT) for s in range(t, NT)]
    rows6 = []
    for t, s in pairs:
        prod = res[t] * res[s]
        for li in range(1, NL):
            prod = prod + res[NT * li + t] * res[NT * li + s]
        rows6.append(jnp.sum(prod, axis=0, keepdims=True))
    tile = jnp.concatenate(rows6 + [jnp.zeros((2, 128), F32)], axis=0) * (inv_tokens * inv_tokens)

    row_id, plane_id = 2 * pos[0] + core, 4 * pos[2] + pos[1]
    gcore[row_id] = tile
    share(row_peers, gcore.at[row_id], gc_s, gc_r)
    tile = tree_sum([gcore[i] for i in range(8)])
    gax[plane_id] = tile
    share(plane_peers, gax.at[plane_id], gx_s, gx_r)
    tile = tree_sum([gax[i] for i in range(16)])

    sums = jnp.broadcast_to(jnp.sum(tile, axis=1, keepdims=True), (8, LN))
    gram = {}
    for i, (t, s) in enumerate(pairs):
        gram[t, s] = gram[s, t] = jnp.broadcast_to(sums[i:i + 1, :], (8, LN))
    temperature = (gram[0, 0] + gram[1, 1] + gram[2, 2]) / NT
    alpha = [jnp.full((8, LN), 1.0 / NT, F32)] * NT

    def eg_step(i, alpha):
        pull = [gram[t, 0] * alpha[0] + gram[t, 1] * alpha[1] + gram[t, 2] * alpha[2] for t in range(NT)]
        new = [alpha[t] * jnp.exp(-pull[t] / temperature) for t in range(NT)]
        total = new[0] + new[1] + new[2]
        return tuple(a / total for a in new)

    alpha = lax.fori_loop(0, EG_STEPS, eg_step, tuple(alpha))
    for t in range(NT):
        alpha_ref[t] = alpha[t][0, 0]
        for s in range(NT):
            gram_ref[t, s] = gram[t, s][0, 0]
    scale = [jnp.broadcast_to(alpha[t][0:1, :] * inv_tokens, (72, 128)) for t in range(NT)]
    for layer in range(NL):
        u = NT * (NL - 1 - layer)
        mix[72 * layer:72 * (layer + 1), :] = scale[0] * res[u] + scale[1] * res[u + 1] + scale[2] * res[u + 2]
    for k in range(36):
        up_ref[:, LN * k:LN * (k + 1)] = mix[pl.ds(k, NL, stride=ROWS), :]
        down_ref[:, LN * k:LN * (k + 1)] = mix[pl.ds(36 + k, NL, stride=ROWS), :]


def whole_step(x, labels, w_up, w_down, heads_t):
    any_spec = pl.BlockSpec(memory_space=pl.ANY)
    vmem_spec = pl.BlockSpec(memory_space=pltpu.VMEM)
    smem_spec = pl.BlockSpec(memory_space=pltpu.SMEM)
    dma = pltpu.SemaphoreType.DMA
    two, three = (2,), (3,)

    def vmem(*shape, dtype=F32):
        return pltpu.VMEM(shape, dtype)

    both = pltpu.SemaphoreType.DMA(three + three + two)
    triple = dma(three + three + three)
    scratch = [
        vmem(2, DF, TOK, dtype=BF16),
        vmem(2, DM, TOK, dtype=BF16),
        vmem(2, TOK, DF),
        vmem(2, DM, DF, dtype=BF16),
        vmem(2, DF, DM, dtype=BF16),
        vmem(TOK, DM, dtype=BF16),
        vmem(NT, TOK, DM, dtype=BF16),
        vmem(TOK, DF, dtype=BF16),
        vmem(BLK, BLK, dtype=BF16),
        vmem(2, 3, DM, LN),
        vmem(3, *GRID, ROWS, LN),
        vmem(2, *GRID, ROWS, LN),
        vmem(2, *GRID, ROWS, LN),
        vmem(3, 3, 2, 2, 4, GRP, LN),
        vmem(3, 3, 2, 4, 4, GRP, LN),
        vmem(3, 3, 4, 4, GRP, LN),
        vmem(3, 3, 2, 2, GRP, LN),
        vmem(3, 3, 2, 4, GRP, LN),
        vmem(3, 3, 4, GRP, LN),
        vmem(3, 3, 3, GRP, LN),
        vmem(UNITS, ROWS, LN),
        vmem(NL * ROWS, LN),
        vmem(8, 8, LN),
        vmem(16, 8, LN),
        dma, dma(two + two), dma(three + two), dma(three + two), dma(two), dma(two),
        both, both, both, both, both, both, both, both,
        triple, triple, both, both, both, both, dma((7,)), dma((7,)), dma((15,)), dma((15,)),
    ]
    return pl.pallas_call(
        step_kernel,
        out_shape=(
            jax.ShapeDtypeStruct((NT,), F32),
            jax.ShapeDtypeStruct((NT, NT), F32),
            jax.ShapeDtypeStruct((NL, HALF * LN), F32),
            jax.ShapeDtypeStruct((NL, HALF * LN), F32),
            jax.ShapeDtypeStruct((2, DF, TOK), BF16),
            jax.ShapeDtypeStruct((2, DM, TOK), BF16),
            jax.ShapeDtypeStruct((2, TOK, DF), F32),
        ),
        in_specs=[any_spec, vmem_spec, any_spec, any_spec, vmem_spec],
        out_specs=(smem_spec, smem_spec, vmem_spec, vmem_spec, any_spec, any_spec, any_spec),
        scratch_shapes=scratch,
        compiler_params=pltpu.CompilerParams(
            collective_id=0, has_side_effects=True, vmem_limit_bytes=67043328),
    )(x, labels, w_up, w_down, heads_t)[:4]


def solution(mesh):
    def local_step(x_local, lab_local, w_up, w_down, task_heads):
        heads_t = jnp.pad(jnp.swapaxes(task_heads, 1, 2), ((0, 0), (0, 16 - NC), (0, 0))).reshape(NT * 16, DM)
        return whole_step(x_local, lab_local, w_up, w_down, heads_t)

    return jax.shard_map(local_step, mesh=mesh, in_specs=(P('data', None), P(None, 'data'), P(), P(), P()), out_specs=(P(), P(), P(None, 'data'), P(None, 'data')), check_vma=False)
```

```python
import jax
import jax.numpy as jnp
from jax import lax
from jax.experimental import pallas as pl
from jax.experimental.pallas import tpu as pltpu
from jax.sharding import PartitionSpec as P

EG_STEPS = 20
NT = 3
NL = 4
DM = 384
DF = 1536
TOK = 1024
NC = 13
LN = 128
ROWS = 72
HALF = 36
GRP = 24
BLK = 256
GRID = (4, 4, 4)
GELU_C = 0.7978845608028654
GELU_K = 0.044715
UNITS = NT * NL
DUE = (5, 8, 11, 14, 17, 20)
AXIS_STRIDE = (2, 8, 32)
MESH = pl.DeviceIdType.MESH
F32 = jnp.float32
BF16 = jnp.bfloat16


def half_slice(half):
    return slice(None) if half is None else pl.ds(2 * half, 2)


def step_kernel(x_hbm, lab_ref, w1_hbm, w2_hbm, heads_ref,
                alpha_ref, gram_ref, up_ref, down_ref, at_save, ht_save, sl_save,
                at, ht, sl, w1, w2, hbuf, dbuf, sbuf, tmp,
                gown, gsend, rd2d, ra1, rb1, acc2, ra2, rb2, acc3, r3, res, mix, gcore, gax,
                x_sem, w_sem, save_sem, load_sem, d2d_s, d2d_r, a1_s, a1_r, b1_s, b1_r,
                a2_s, a2_r, b2_s, b2_r, c3_s, c3_r, e1_s, e1_r, e2_s, e2_r, gc_s, gc_r, gx_s, gx_r):
    me = lax.axis_index('data')
    core = lax.rem(me, 2)
    pos = [lax.rem(me // s, 4) for s in AXIS_STRIDE]
    sibling = me + 1 - 2 * core

    def at_pos(axis, k):
        return lax.rem(pos[axis] + k, 4)

    def peer(axis, k):
        return me + (at_pos(axis, k) - pos[axis]) * AXIS_STRIDE[axis]

    barrier = pltpu.get_barrier_semaphore()
    row_peers = [sibling] + [dev + c * (sibling - me) for dev in (peer(0, 1), peer(0, 2), peer(0, 3)) for c in range(2)]
    plane_peers = [me + peer(1, j) - me + peer(2, k) - me for k in range(4) for j in range(4) if j + k]
    partners = row_peers + plane_peers
    for dev in partners:
        pl.semaphore_signal(barrier, inc=1, device_id=(dev,), device_id_type=MESH)

    def w_loads(layer, slot):
        return [pltpu.make_async_copy(w1_hbm.at[layer], w1.at[slot], w_sem.at[0, slot]),
                pltpu.make_async_copy(w2_hbm.at[layer], w2.at[slot], w_sem.at[1, slot])]

    def saves(layer):
        return [pltpu.make_async_copy(at.at[layer], at_save.at[layer], save_sem.at[0, layer]),
                pltpu.make_async_copy(ht.at[layer], ht_save.at[layer], save_sem.at[1, layer]),
                pltpu.make_async_copy(sl.at[layer], sl_save.at[layer], save_sem.at[2, layer])]

    def loads(layer):
        return [pltpu.make_async_copy(at_save.at[layer], at.at[layer], load_sem.at[0, layer]),
                pltpu.make_async_copy(ht_save.at[layer], ht.at[layer], load_sem.at[1, layer]),
                pltpu.make_async_copy(sl_save.at[layer], sl.at[layer], load_sem.at[2, layer])] + w_loads(layer, layer)

    x_load = pltpu.make_async_copy(x_hbm, hbuf, x_sem)
    x_load.start()
    for cp in w_loads(0, 0):
        cp.start()
    x_load.wait()

    def nt_dot(a, b):
        return lax.dot_general(a, b, (((1,), (1,)), ((), ())), preferred_element_type=F32)

    def forward(layer, carry):
        slot = lax.rem(layer, 2)
        for cp in w_loads(layer, slot):
            cp.wait()

        @pl.when(layer < NL - 1)
        def _():
            for cp in w_loads(layer + 1, 1 - slot):
                cp.start()

        @pl.when(layer >= 2)
        def _():
            for cp in saves(layer - 2):
                cp.wait()

        for n in range(3):
            ht[slot, LN * n:LN * (n + 1), :] = hbuf[:, LN * n:LN * (n + 1)].T

        def up(mb, c):
            rows = slice(None)
            for n in range(6):
                cols = slice(BLK * n, BLK * (n + 1))
                x = jnp.dot(hbuf[rows, :], w1[slot, :, cols], preferred_element_type=F32)
                x2 = x * x
                th = jnp.tanh(x * (GELU_C + (GELU_C * GELU_K) * x2))
                hp = 0.5 + 0.5 * th
                act = x * hp
                sbuf[rows, cols] = act.astype(BF16)
                sl[slot, rows, cols] = hp + act * ((1.0 - th) * (GELU_C + (3.0 * GELU_C * GELU_K) * x2))
            return c

        up(0, 0)
        for n in range(6):
            cols = slice(BLK * n, BLK * (n + 1))
            at[slot, cols, :] = sbuf[:, cols].T

        @pl.when(layer < 2)
        def _():
            for cp in saves(layer):
                cp.start()

        def down(mb, c):
            rows = slice(None)
            val = jnp.dot(sbuf[rows, :], w2[slot], preferred_element_type=F32)
            hbuf[rows, :] = (hbuf[rows, :].astype(F32) + val).astype(BF16)
            return c

        down(0, 0)
        return carry

    lax.fori_loop(0, NL, forward, 0)

    logits = nt_dot(heads_ref[...], hbuf[...])
    class_id = lax.broadcasted_iota(jnp.int32, (16, TOK), 0)
    for t in range(NT):
        lg = jnp.where(class_id < NC, logits[16 * t:16 * (t + 1), :], -jnp.inf)
        ex = jnp.exp(lg - jnp.max(lg, axis=0, keepdims=True))
        prob = ex / jnp.sum(ex, axis=0, keepdims=True)
        onehot = (class_id == lab_ref[t:t + 1, :]).astype(F32)
        err = jnp.transpose(prob - onehot).astype(BF16)
        dbuf[t] = jnp.dot(err, heads_ref[16 * t:16 * (t + 1), :], preferred_element_type=F32).astype(BF16)

    pl.semaphore_wait(barrier, len(partners))

    def remote(src, dst, send, recv, dev):
        return pltpu.make_async_remote_copy(
            src_ref=src, dst_ref=dst, send_sem=send, recv_sem=recv,
            device_id=(dev,), device_id_type=MESH)

    def chunk1(g3, p, idx, half=None):
        h, rows = half_slice(half), pl.ds(24 * p, 24)
        return (gown.at[g3, h, :, idx, rows, :], gown.at[g3, h, idx, :, rows, :],
                gown.at[g3, idx, h, :, rows, :])[p]

    def chunk2(par, p, idx, half=None):
        h = half_slice(half)
        return (acc2.at[par, 0, h, idx], acc2.at[par, 1, idx, h], acc2.at[par, 2, h, idx])[p]

    def d2d_copies(v):
        par = lax.rem(v, 2)
        part = [(par, slice(None), slice(None), slice(None), pl.ds(GRP * p, GRP)) for p in range(3)]
        return [remote(gsend.at[part[p]], rd2d.at[part[p]], d2d_s.at[par, p], d2d_r.at[par, p], sibling) for p in range(3)]

    def relay1(v):
        par = g3 = lax.rem(v, 3)
        return [remote(chunk1(g3, p, at_pos(p, 2), d), ra1.at[par, p, d], a1_s.at[par, p, d],
                       a1_r.at[par, p, d], peer(p, 1 + 2 * d)) for p in range(3) for d in range(2)]

    def direct1(v):
        par = g3 = lax.rem(v, 3)
        return [remote(chunk1(g3, p, at_pos(p, 1 + 2 * d), 1 - d), rb1.at[par, p, d, half_slice(1 - d)],
                       e1_s.at[par, p, d], e1_r.at[par, p, d], peer(p, 1 + 2 * d)) for p in range(3) for d in range(2)]

    def main1(v):
        par = g3 = lax.rem(v, 3)
        return [remote(chunk1(g3, p, at_pos(p, 1 + 2 * d), d), rb1.at[par, p, d, half_slice(d)], b1_s.at[par, p, d],
                       b1_r.at[par, p, d], peer(p, 1 + 2 * d)) for p in range(3) for d in range(2)]

    def relay2(v):
        par = lax.rem(v, 3)
        return [remote(chunk2(par, p, at_pos((p + 1) % 3, 2), d), ra2.at[par, p, d], a2_s.at[par, p, d],
                       a2_r.at[par, p, d], peer((p + 1) % 3, 1 + 2 * d)) for p in range(3) for d in range(2)]

    def direct2(v):
        par = lax.rem(v, 3)
        return [remote(chunk2(par, p, at_pos((p + 1) % 3, 1 + 2 * d), 1 - d), rb2.at[par, p, d, half_slice(1 - d)],
                       e2_s.at[par, p, d], e2_r.at[par, p, d], peer((p + 1) % 3, 1 + 2 * d))
                for p in range(3) for d in range(2)]

    def main2(v):
        par = lax.rem(v, 3)
        return [remote(chunk2(par, p, at_pos((p + 1) % 3, 1 + 2 * d), d), rb2.at[par, p, d, half_slice(d)],
                       b2_s.at[par, p, d], b2_r.at[par, p, d], peer((p + 1) % 3, 1 + 2 * d))
                for p in range(3) for d in range(2)]

    def last3(v):
        par = lax.rem(v, 3)
        return [remote(acc3.at[par, p, at_pos((p + 2) % 3, k)], r3.at[par, p, k - 1], c3_s.at[par, p, k - 1],
                       c3_r.at[par, p, k - 1], peer((p + 2) % 3, k)) for p in range(3) for k in (1, 2, 3)]

    def share(peers, slot, send, recv):
        copies = [remote(slot, slot, send.at[i], recv.at[i], dev) for i, dev in enumerate(peers)]
        for cp in copies:
            cp.start()
        for cp in copies:
            cp.wait()

    def tree_sum(terms):
        while len(terms) > 1:
            terms = [a + b for a, b in zip(terms[::2], terms[1::2])]
        return terms[0]

    def start(copies):
        for cp in copies:
            cp.start()

    def wait(copies):
        for cp in copies:
            cp.wait()

    def step_d2d(v):
        par, g3 = lax.rem(v, 2), lax.rem(v, 3)
        relays, directs = relay1(v), direct1(v)
        for p, cp in enumerate(d2d_copies(v)):
            cp.wait()

            def add(i, carry, p=p):
                rows = pl.ds(GRP * p, GRP)
                gown[g3, i, :, :, rows, :] = gown[g3, i, :, :, rows, :] + rd2d[par, i, :, :, rows, :]
                return carry

            lax.fori_loop(0, 4, add, 0)
            start(relays[2 * p:2 * p + 2])
        start(directs)

    def step_relay1(v):
        par = g3 = lax.rem(v, 3)
        relays, mains = relay1(v), main1(v)
        for p in range(3):
            for d in range(2):
                relays[2 * p + d].wait()
                dst = chunk1(g3, p, at_pos(p, 1 + 2 * d), d)
                dst[...] = dst[...] + ra1[par, p, d]
                mains[2 * p + d].start()

    def step_main1(v):
        par = g3 = lax.rem(v, 3)
        mains, early, relays, directs = main1(v), direct1(v), relay2(v), direct2(v)
        for p in range(3):
            pair = slice(2 * p, 2 * p + 2)
            wait(early[pair] + mains[pair])
            acc2[par, p] = chunk1(g3, p, pos[p])[...] + rb1[par, p, 0] + rb1[par, p, 1]
            start(relays[pair])
        start(directs)

    def step_relay2(v):
        par = lax.rem(v, 3)
        relays, mains = relay2(v), main2(v)
        for p in range(3):
            for d in range(2):
                relays[2 * p + d].wait()
                dst = chunk2(par, p, at_pos((p + 1) % 3, 1 + 2 * d), d)
                dst[...] = dst[...] + ra2[par, p, d]
                mains[2 * p + d].start()

    def step_main2(v):
        par = lax.rem(v, 3)
        mains, early, lasts = main2(v), direct2(v), last3(v)
        for p in range(3):
            pair = slice(2 * p, 2 * p + 2)
            wait(early[pair] + mains[pair])
            acc3[par, p] = chunk2(par, p, pos[(p + 1) % 3])[...] + rb2[par, p, 0] + rb2[par, p, 1]
            start(lasts[3 * p:3 * p + 3])

    def step_last3(v):
        wait(last3(v))
        par = lax.rem(v, 3)
        for p in range(3):
            res[v, pl.ds(24 * p, 24), :] = (
                (acc3[par, p, pos[(p + 2) % 3]] + r3[par, p, 0]) + (r3[par, p, 1] + r3[par, p, 2]))

    def when_unit(v, step):
        pl.when(jnp.logical_and(v >= 0, v < UNITS))(lambda: step(v))

    steps = (step_d2d, step_relay1, step_main1, step_relay2, step_main2, step_last3)

    def run_slot(u, k):
        for due, step in reversed(tuple(zip(DUE, steps))):
            if due % 4 == k:
                when_unit(u - due // 4, step)

    def body(u, carry):
        li, task = u // NT, lax.rem(u, NT)
        slot = lax.rem(li + 1, 2)
        par, g3 = lax.rem(u, 2), lax.rem(u, 3)
        computing = u < UNITS

        def dest(rel):
            if rel == 0:
                return gown.at[g3].reshape(64 * ROWS, LN)
            return gsend.at[par].reshape(64 * ROWS, LN)

        for k in (2, 3):
            @pl.when(u == NT * (k - 1))
            def _(k=k):
                for cp in loads(NL - 1 - k):
                    cp.start()

            @pl.when(u == NT * k)
            def _(k=k):
                for cp in loads(NL - 1 - k):
                    cp.wait()

        @pl.when(computing)
        def _():
            for m in range(4):
                val = jnp.dot(at[slot, 384 * m:384 * (m + 1), :], dbuf[task], preferred_element_type=F32)
                for lb in range(3):
                    tmp[m % 2, lb] = val[:, LN * lb:LN * (lb + 1)]
                for rel in range(2):
                    cc = core if rel == 0 else 1 - core
                    dst = dest(rel)
                    for j in range(12):
                        for lb in range(3):
                            dst[pl.ds(m * 16 * 72 + 36 + 3 * j + lb, 16, stride=ROWS), :] = (
                                tmp[m % 2, lb, pl.ds(12 * cc + j, 16, stride=24), :])

        run_slot(u, 0)

        @pl.when(computing)
        def _():
            def block(mb, c):
                rows = slice(None)
                for n in range(6):
                    cols = slice(BLK * n, BLK * (n + 1))
                    val = nt_dot(dbuf[task, rows, :], w2[slot, cols, :])
                    sbuf[rows, cols] = (val * sl[slot, rows, cols]).astype(BF16)
                return c
            block(0, 0)

        run_slot(u, 1)

        @pl.when(computing)
        def _():
            for n in range(6):
                val = jnp.dot(ht[slot], sbuf[:, BLK * n:BLK * (n + 1)], preferred_element_type=F32)
                for lb in range(2):
                    tmp[n % 2, lb] = val[:, LN * lb:LN * (lb + 1)]
                for rel in range(2):
                    cc = core if rel == 0 else 1 - core
                    dst = dest(rel)
                    for r in range(3):
                        for lb in range(2):
                            dst[pl.ds(12 * r + 2 * n + lb, 64, stride=ROWS), :] = (
                                tmp[n % 2, lb, pl.ds(3 * cc + r, 64, stride=6), :])

        when_unit(u, lambda v: start(d2d_copies(v)))
        run_slot(u, 2)

        @pl.when(u < UNITS - NT)
        def _():
            def block(mb, c):
                rows = slice(None)
                val = nt_dot(sbuf[rows, :], w1[slot])
                dbuf[task, rows, :] = (dbuf[task, rows, :].astype(F32) + val).astype(BF16)
                return c
            block(0, 0)

        run_slot(u, 3)
        return carry

    lax.fori_loop(0, UNITS + DUE[-1] // 4, body, 0)

    inv_tokens = 1.0 / (TOK * lax.axis_size('data'))
    pairs = [(t, s) for t in range(NT) for s in range(t, NT)]
    rows6 = []
    for t, s in pairs:
        prod = res[t] * res[s]
        for li in range(1, NL):
            prod = prod + res[NT * li + t] * res[NT * li + s]
        rows6.append(jnp.sum(prod, axis=0, keepdims=True))
    tile = jnp.concatenate(rows6 + [jnp.zeros((2, 128), F32)], axis=0) * (inv_tokens * inv_tokens)

    row_id, plane_id = 2 * pos[0] + core, 4 * pos[2] + pos[1]
    gcore[row_id] = tile
    share(row_peers, gcore.at[row_id], gc_s, gc_r)
    tile = tree_sum([gcore[i] for i in range(8)])
    gax[plane_id] = tile
    share(plane_peers, gax.at[plane_id], gx_s, gx_r)
    tile = tree_sum([gax[i] for i in range(16)])

    sums = jnp.broadcast_to(jnp.sum(tile, axis=1, keepdims=True), (8, LN))
    gram = {}
    for i, (t, s) in enumerate(pairs):
        gram[t, s] = gram[s, t] = jnp.broadcast_to(sums[i:i + 1, :], (8, LN))
    temperature = (gram[0, 0] + gram[1, 1] + gram[2, 2]) / NT
    alpha = [jnp.full((8, LN), 1.0 / NT, F32)] * NT

    def eg_step(i, alpha):
        pull = [gram[t, 0] * alpha[0] + gram[t, 1] * alpha[1] + gram[t, 2] * alpha[2] for t in range(NT)]
        new = [alpha[t] * jnp.exp(-pull[t] / temperature) for t in range(NT)]
        total = new[0] + new[1] + new[2]
        return tuple(a / total for a in new)

    alpha = lax.fori_loop(0, EG_STEPS, eg_step, tuple(alpha))
    for t in range(NT):
        alpha_ref[t] = alpha[t][0, 0]
        for s in range(NT):
            gram_ref[t, s] = gram[t, s][0, 0]
    scale = [jnp.broadcast_to(alpha[t][0:1, :] * inv_tokens, (72, 128)) for t in range(NT)]
    for layer in range(NL):
        u = NT * (NL - 1 - layer)
        mix[72 * layer:72 * (layer + 1), :] = scale[0] * res[u] + scale[1] * res[u + 1] + scale[2] * res[u + 2]
    for k in range(36):
        up_ref[:, LN * k:LN * (k + 1)] = mix[pl.ds(k, NL, stride=ROWS), :]
        down_ref[:, LN * k:LN * (k + 1)] = mix[pl.ds(36 + k, NL, stride=ROWS), :]


def whole_step(x, labels, w_up, w_down, heads_t):
    any_spec = pl.BlockSpec(memory_space=pl.ANY)
    vmem_spec = pl.BlockSpec(memory_space=pltpu.VMEM)
    smem_spec = pl.BlockSpec(memory_space=pltpu.SMEM)
    dma = pltpu.SemaphoreType.DMA
    two, three = (2,), (3,)

    def vmem(*shape, dtype=F32):
        return pltpu.VMEM(shape, dtype)

    both = pltpu.SemaphoreType.DMA(three + three + two)
    triple = dma(three + three + three)
    scratch = [
        vmem(2, DF, TOK, dtype=BF16),
        vmem(2, DM, TOK, dtype=BF16),
        vmem(2, TOK, DF),
        vmem(2, DM, DF, dtype=BF16),
        vmem(2, DF, DM, dtype=BF16),
        vmem(TOK, DM, dtype=BF16),
        vmem(NT, TOK, DM, dtype=BF16),
        vmem(TOK, DF, dtype=BF16),
        vmem(2, 3, DM, LN),
        vmem(3, *GRID, ROWS, LN),
        vmem(2, *GRID, ROWS, LN),
        vmem(2, *GRID, ROWS, LN),
        vmem(3, 3, 2, 2, 4, GRP, LN),
        vmem(3, 3, 2, 4, 4, GRP, LN),
        vmem(3, 3, 4, 4, GRP, LN),
        vmem(3, 3, 2, 2, GRP, LN),
        vmem(3, 3, 2, 4, GRP, LN),
        vmem(3, 3, 4, GRP, LN),
        vmem(3, 3, 3, GRP, LN),
        vmem(UNITS, ROWS, LN),
        vmem(NL * ROWS, LN),
        vmem(8, 8, LN),
        vmem(16, 8, LN),
        dma, dma(two + two), dma(three + two), dma(three + two), dma(two + three), dma(two + three),
        both, both, both, both, both, both, both, both,
        triple, triple, both, both, both, both, dma((7,)), dma((7,)), dma((15,)), dma((15,)),
    ]
    return pl.pallas_call(
        step_kernel,
        out_shape=(
            jax.ShapeDtypeStruct((NT,), F32),
            jax.ShapeDtypeStruct((NT, NT), F32),
            jax.ShapeDtypeStruct((NL, HALF * LN), F32),
            jax.ShapeDtypeStruct((NL, HALF * LN), F32),
            jax.ShapeDtypeStruct((2, DF, TOK), BF16),
            jax.ShapeDtypeStruct((2, DM, TOK), BF16),
            jax.ShapeDtypeStruct((2, TOK, DF), F32),
        ),
        in_specs=[any_spec, vmem_spec, any_spec, any_spec, vmem_spec],
        out_specs=(smem_spec, smem_spec, vmem_spec, vmem_spec, any_spec, any_spec, any_spec),
        scratch_shapes=scratch,
        compiler_params=pltpu.CompilerParams(
            collective_id=0, has_side_effects=True, vmem_limit_bytes=67043328),
    )(x, labels, w_up, w_down, heads_t)[:4]


def solution(mesh):
    def local_step(x_local, lab_local, w_up, w_down, task_heads):
        heads_t = jnp.pad(jnp.swapaxes(task_heads, 1, 2), ((0, 0), (0, 16 - NC), (0, 0))).reshape(NT * 16, DM)
        return whole_step(x_local, lab_local, w_up, w_down, heads_t)

    return jax.shard_map(local_step, mesh=mesh, in_specs=(P('data', None), P(None, 'data'), P(), P(), P()), out_specs=(P(), P(), P(None, 'data'), P(None, 'data')), check_vma=False)
```

```python
import jax
import jax.numpy as jnp
from jax import lax
from jax.experimental import pallas as pl
from jax.experimental.pallas import tpu as pltpu
from jax.sharding import PartitionSpec as P

EG_STEPS = 20
NT = 3
NL = 4
DM = 384
DF = 1536
TOK = 1024
NC = 13
LN = 128
ROWS = 72
HALF = 36
GRP = 24
BLK = 256
GRID = (4, 4, 4)
GELU_C = 0.7978845608028654
GELU_K = 0.044715
UNITS = NT * NL
DUE = (5, 8, 11, 14, 17, 20)
AXIS_STRIDE = (2, 8, 32)
MESH = pl.DeviceIdType.MESH
F32 = jnp.float32
BF16 = jnp.bfloat16


def half_slice(half):
    return slice(None) if half is None else pl.ds(2 * half, 2)


def step_kernel(x_hbm, lab_ref, w1_hbm, w2_hbm, heads_ref,
                pack_ref, at_save, ht_save, sl_save,
                at, ht, sl, w1, w2, hbuf, dbuf, sbuf, tmp,
                gown, gsend, rd2d, ra1, rb1, acc2, ra2, rb2, acc3, r3, res, mix, gcore, gax,
                x_sem, w_sem, save_sem, load_sem, d2d_s, d2d_r, a1_s, a1_r, b1_s, b1_r,
                a2_s, a2_r, b2_s, b2_r, c3_s, c3_r, e1_s, e1_r, e2_s, e2_r, gc_s, gc_r, gx_s, gx_r):
    me = lax.axis_index('data')
    core = lax.rem(me, 2)
    pos = [lax.rem(me // s, 4) for s in AXIS_STRIDE]
    sibling = me + 1 - 2 * core

    def at_pos(axis, k):
        return lax.rem(pos[axis] + k, 4)

    def peer(axis, k):
        return me + (at_pos(axis, k) - pos[axis]) * AXIS_STRIDE[axis]

    barrier = pltpu.get_barrier_semaphore()
    row_peers = [sibling] + [dev + c * (sibling - me) for dev in (peer(0, 1), peer(0, 2), peer(0, 3)) for c in range(2)]
    plane_peers = [me + peer(1, j) - me + peer(2, k) - me for k in range(4) for j in range(4) if j + k]
    partners = row_peers + plane_peers
    for dev in partners:
        pl.semaphore_signal(barrier, inc=1, device_id=(dev,), device_id_type=MESH)

    def w_loads(layer, slot):
        return [pltpu.make_async_copy(w1_hbm.at[layer], w1.at[slot], w_sem.at[0, slot]),
                pltpu.make_async_copy(w2_hbm.at[layer], w2.at[slot], w_sem.at[1, slot])]

    def saves(layer):
        return [pltpu.make_async_copy(at.at[layer], at_save.at[layer], save_sem.at[0, layer]),
                pltpu.make_async_copy(ht.at[layer], ht_save.at[layer], save_sem.at[1, layer]),
                pltpu.make_async_copy(sl.at[layer], sl_save.at[layer], save_sem.at[2, layer])]

    def loads(layer):
        return [pltpu.make_async_copy(at_save.at[layer], at.at[layer], load_sem.at[0, layer]),
                pltpu.make_async_copy(ht_save.at[layer], ht.at[layer], load_sem.at[1, layer]),
                pltpu.make_async_copy(sl_save.at[layer], sl.at[layer], load_sem.at[2, layer])] + w_loads(layer, layer)

    x_load = pltpu.make_async_copy(x_hbm, hbuf, x_sem)
    x_load.start()
    for cp in w_loads(0, 0):
        cp.start()
    x_load.wait()

    def nt_dot(a, b):
        return lax.dot_general(a, b, (((1,), (1,)), ((), ())), preferred_element_type=F32)

    def forward(layer, carry):
        slot = lax.rem(layer, 2)
        for cp in w_loads(layer, slot):
            cp.wait()

        @pl.when(layer < NL - 1)
        def _():
            for cp in w_loads(layer + 1, 1 - slot):
                cp.start()

        @pl.when(layer >= 2)
        def _():
            for cp in saves(layer - 2):
                cp.wait()

        for n in range(3):
            ht[slot, LN * n:LN * (n + 1), :] = hbuf[:, LN * n:LN * (n + 1)].T

        def up(mb, c):
            rows = slice(None)
            for n in range(6):
                cols = slice(BLK * n, BLK * (n + 1))
                x = jnp.dot(hbuf[rows, :], w1[slot, :, cols], preferred_element_type=F32)
                x2 = x * x
                th = jnp.tanh(x * (GELU_C + (GELU_C * GELU_K) * x2))
                hp = 0.5 + 0.5 * th
                act = x * hp
                sbuf[rows, cols] = act.astype(BF16)
                sl[slot, rows, cols] = hp + act * ((1.0 - th) * (GELU_C + (3.0 * GELU_C * GELU_K) * x2))
            return c

        up(0, 0)
        for n in range(6):
            cols = slice(BLK * n, BLK * (n + 1))
            at[slot, cols, :] = sbuf[:, cols].T

        @pl.when(layer < 2)
        def _():
            for cp in saves(layer):
                cp.start()

        def down(mb, c):
            rows = slice(None)
            val = jnp.dot(sbuf[rows, :], w2[slot], preferred_element_type=F32)
            hbuf[rows, :] = (hbuf[rows, :].astype(F32) + val).astype(BF16)
            return c

        down(0, 0)
        return carry

    lax.fori_loop(0, NL, forward, 0)

    logits = nt_dot(heads_ref[...], hbuf[...])
    class_id = lax.broadcasted_iota(jnp.int32, (16, TOK), 0)
    for t in range(NT):
        lg = jnp.where(class_id < NC, logits[16 * t:16 * (t + 1), :], -jnp.inf)
        ex = jnp.exp(lg - jnp.max(lg, axis=0, keepdims=True))
        prob = ex / jnp.sum(ex, axis=0, keepdims=True)
        onehot = (class_id == lab_ref[t:t + 1, :]).astype(F32)
        err = jnp.transpose(prob - onehot).astype(BF16)
        dbuf[t] = jnp.dot(err, heads_ref[16 * t:16 * (t + 1), :], preferred_element_type=F32).astype(BF16)

    pl.semaphore_wait(barrier, len(partners))

    def remote(src, dst, send, recv, dev):
        return pltpu.make_async_remote_copy(
            src_ref=src, dst_ref=dst, send_sem=send, recv_sem=recv,
            device_id=(dev,), device_id_type=MESH)

    def chunk1(g3, p, idx, half=None):
        h, rows = half_slice(half), pl.ds(24 * p, 24)
        return (gown.at[g3, h, :, idx, rows, :], gown.at[g3, h, idx, :, rows, :],
                gown.at[g3, idx, h, :, rows, :])[p]

    def chunk2(par, p, idx, half=None):
        h = half_slice(half)
        return (acc2.at[par, 0, h, idx], acc2.at[par, 1, idx, h], acc2.at[par, 2, h, idx])[p]

    def d2d_copies(v):
        par = lax.rem(v, 2)
        part = [(par, slice(None), slice(None), slice(None), pl.ds(GRP * p, GRP)) for p in range(3)]
        return [remote(gsend.at[part[p]], rd2d.at[part[p]], d2d_s.at[par, p], d2d_r.at[par, p], sibling) for p in range(3)]

    def relay1(v):
        par = g3 = lax.rem(v, 3)
        return [remote(chunk1(g3, p, at_pos(p, 2), d), ra1.at[par, p, d], a1_s.at[par, p, d],
                       a1_r.at[par, p, d], peer(p, 1 + 2 * d)) for p in range(3) for d in range(2)]

    def direct1(v):
        par = g3 = lax.rem(v, 3)
        return [remote(chunk1(g3, p, at_pos(p, 1 + 2 * d), 1 - d), rb1.at[par, p, d, half_slice(1 - d)],
                       e1_s.at[par, p, d], e1_r.at[par, p, d], peer(p, 1 + 2 * d)) for p in range(3) for d in range(2)]

    def main1(v):
        par = g3 = lax.rem(v, 3)
        return [remote(chunk1(g3, p, at_pos(p, 1 + 2 * d), d), rb1.at[par, p, d, half_slice(d)], b1_s.at[par, p, d],
                       b1_r.at[par, p, d], peer(p, 1 + 2 * d)) for p in range(3) for d in range(2)]

    def relay2(v):
        par = lax.rem(v, 3)
        return [remote(chunk2(par, p, at_pos((p + 1) % 3, 2), d), ra2.at[par, p, d], a2_s.at[par, p, d],
                       a2_r.at[par, p, d], peer((p + 1) % 3, 1 + 2 * d)) for p in range(3) for d in range(2)]

    def direct2(v):
        par = lax.rem(v, 3)
        return [remote(chunk2(par, p, at_pos((p + 1) % 3, 1 + 2 * d), 1 - d), rb2.at[par, p, d, half_slice(1 - d)],
                       e2_s.at[par, p, d], e2_r.at[par, p, d], peer((p + 1) % 3, 1 + 2 * d))
                for p in range(3) for d in range(2)]

    def main2(v):
        par = lax.rem(v, 3)
        return [remote(chunk2(par, p, at_pos((p + 1) % 3, 1 + 2 * d), d), rb2.at[par, p, d, half_slice(d)],
                       b2_s.at[par, p, d], b2_r.at[par, p, d], peer((p + 1) % 3, 1 + 2 * d))
                for p in range(3) for d in range(2)]

    def last3(v):
        par = lax.rem(v, 3)
        return [remote(acc3.at[par, p, at_pos((p + 2) % 3, k)], r3.at[par, p, k - 1], c3_s.at[par, p, k - 1],
                       c3_r.at[par, p, k - 1], peer((p + 2) % 3, k)) for p in range(3) for k in (1, 2, 3)]

    def share(peers, slot, send, recv):
        copies = [remote(slot, slot, send.at[i], recv.at[i], dev) for i, dev in enumerate(peers)]
        for cp in copies:
            cp.start()
        for cp in copies:
            cp.wait()

    def tree_sum(terms):
        while len(terms) > 1:
            terms = [a + b for a, b in zip(terms[::2], terms[1::2])]
        return terms[0]

    def start(copies):
        for cp in copies:
            cp.start()

    def wait(copies):
        for cp in copies:
            cp.wait()

    def step_d2d(v):
        par, g3 = lax.rem(v, 2), lax.rem(v, 3)
        relays, directs = relay1(v), direct1(v)
        for p, cp in enumerate(d2d_copies(v)):
            cp.wait()

            def add(i, carry, p=p):
                rows = pl.ds(GRP * p, GRP)
                gown[g3, i, :, :, rows, :] = gown[g3, i, :, :, rows, :] + rd2d[par, i, :, :, rows, :]
                return carry

            lax.fori_loop(0, 4, add, 0)
            start(relays[2 * p:2 * p + 2])
        start(directs)

    def step_relay1(v):
        par = g3 = lax.rem(v, 3)
        relays, mains = relay1(v), main1(v)
        for p in range(3):
            for d in range(2):
                relays[2 * p + d].wait()
                dst = chunk1(g3, p, at_pos(p, 1 + 2 * d), d)
                dst[...] = dst[...] + ra1[par, p, d]
                mains[2 * p + d].start()

    def step_main1(v):
        par = g3 = lax.rem(v, 3)
        mains, early, relays, directs = main1(v), direct1(v), relay2(v), direct2(v)
        for p in range(3):
            pair = slice(2 * p, 2 * p + 2)
            wait(early[pair] + mains[pair])
            acc2[par, p] = chunk1(g3, p, pos[p])[...] + rb1[par, p, 0] + rb1[par, p, 1]
            start(relays[pair])
        start(directs)

    def step_relay2(v):
        par = lax.rem(v, 3)
        relays, mains = relay2(v), main2(v)
        for p in range(3):
            for d in range(2):
                relays[2 * p + d].wait()
                dst = chunk2(par, p, at_pos((p + 1) % 3, 1 + 2 * d), d)
                dst[...] = dst[...] + ra2[par, p, d]
                mains[2 * p + d].start()

    def step_main2(v):
        par = lax.rem(v, 3)
        mains, early, lasts = main2(v), direct2(v), last3(v)
        for p in range(3):
            pair = slice(2 * p, 2 * p + 2)
            wait(early[pair] + mains[pair])
            acc3[par, p] = chunk2(par, p, pos[(p + 1) % 3])[...] + rb2[par, p, 0] + rb2[par, p, 1]
            start(lasts[3 * p:3 * p + 3])

    def step_last3(v):
        wait(last3(v))
        par = lax.rem(v, 3)
        for p in range(3):
            res[v, pl.ds(24 * p, 24), :] = (
                (acc3[par, p, pos[(p + 2) % 3]] + r3[par, p, 0]) + (r3[par, p, 1] + r3[par, p, 2]))

    def when_unit(v, step):
        pl.when(jnp.logical_and(v >= 0, v < UNITS))(lambda: step(v))

    steps = (step_d2d, step_relay1, step_main1, step_relay2, step_main2, step_last3)

    def run_slot(u, k):
        for due, step in reversed(tuple(zip(DUE, steps))):
            if due % 4 == k:
                when_unit(u - due // 4, step)

    def body(u, carry):
        li, task = u // NT, lax.rem(u, NT)
        slot = lax.rem(li + 1, 2)
        par, g3 = lax.rem(u, 2), lax.rem(u, 3)
        computing = u < UNITS

        def dest(rel):
            if rel == 0:
                return gown.at[g3].reshape(64 * ROWS, LN)
            return gsend.at[par].reshape(64 * ROWS, LN)

        for k in (2, 3):
            @pl.when(u == NT * (k - 1))
            def _(k=k):
                for cp in loads(NL - 1 - k):
                    cp.start()

            @pl.when(u == NT * k)
            def _(k=k):
                for cp in loads(NL - 1 - k):
                    cp.wait()

        @pl.when(computing)
        def _():
            for m in range(4):
                val = jnp.dot(at[slot, 384 * m:384 * (m + 1), :], dbuf[task], preferred_element_type=F32)
                for lb in range(3):
                    tmp[m % 2, lb] = val[:, LN * lb:LN * (lb + 1)]
                for rel in range(2):
                    cc = core if rel == 0 else 1 - core
                    dst = dest(rel)
                    for j in range(12):
                        for lb in range(3):
                            dst[pl.ds(m * 16 * 72 + 36 + 3 * j + lb, 16, stride=ROWS), :] = (
                                tmp[m % 2, lb, pl.ds(12 * cc + j, 16, stride=24), :])

        run_slot(u, 0)

        @pl.when(computing)
        def _():
            def block(mb, c):
                rows = slice(None)
                for n in range(6):
                    cols = slice(BLK * n, BLK * (n + 1))
                    val = nt_dot(dbuf[task, rows, :], w2[slot, cols, :])
                    sbuf[rows, cols] = (val * sl[slot, rows, cols]).astype(BF16)
                return c
            block(0, 0)

        run_slot(u, 1)

        @pl.when(computing)
        def _():
            for n in range(6):
                val = jnp.dot(ht[slot], sbuf[:, BLK * n:BLK * (n + 1)], preferred_element_type=F32)
                for lb in range(2):
                    tmp[n % 2, lb] = val[:, LN * lb:LN * (lb + 1)]
                for rel in range(2):
                    cc = core if rel == 0 else 1 - core
                    dst = dest(rel)
                    for r in range(3):
                        for lb in range(2):
                            dst[pl.ds(12 * r + 2 * n + lb, 64, stride=ROWS), :] = (
                                tmp[n % 2, lb, pl.ds(3 * cc + r, 64, stride=6), :])

        when_unit(u, lambda v: start(d2d_copies(v)))
        run_slot(u, 2)

        @pl.when(u < UNITS - NT)
        def _():
            def block(mb, c):
                rows = slice(None)
                val = nt_dot(sbuf[rows, :], w1[slot])
                dbuf[task, rows, :] = (dbuf[task, rows, :].astype(F32) + val).astype(BF16)
                return c
            block(0, 0)

        run_slot(u, 3)
        return carry

    lax.fori_loop(0, UNITS + DUE[-1] // 4, body, 0)

    inv_tokens = 1.0 / (TOK * lax.axis_size('data'))
    pairs = [(t, s) for t in range(NT) for s in range(t, NT)]
    rows6 = []
    for t, s in pairs:
        prod = res[t] * res[s]
        for li in range(1, NL):
            prod = prod + res[NT * li + t] * res[NT * li + s]
        rows6.append(jnp.sum(prod, axis=0, keepdims=True))
    tile = jnp.concatenate(rows6 + [jnp.zeros((2, 128), F32)], axis=0) * (inv_tokens * inv_tokens)

    row_id, plane_id = 2 * pos[0] + core, 4 * pos[2] + pos[1]
    gcore[row_id] = tile
    share(row_peers, gcore.at[row_id], gc_s, gc_r)
    tile = tree_sum([gcore[i] for i in range(8)])
    gax[plane_id] = tile
    share(plane_peers, gax.at[plane_id], gx_s, gx_r)
    tile = tree_sum([gax[i] for i in range(16)])

    sums = jnp.broadcast_to(jnp.sum(tile, axis=1, keepdims=True), (8, LN))
    gram = {}
    for i, (t, s) in enumerate(pairs):
        gram[t, s] = gram[s, t] = jnp.broadcast_to(sums[i:i + 1, :], (8, LN))
    temperature = (gram[0, 0] + gram[1, 1] + gram[2, 2]) / NT
    alpha = [jnp.full((8, LN), 1.0 / NT, F32)] * NT

    def eg_step(i, alpha):
        pull = [gram[t, 0] * alpha[0] + gram[t, 1] * alpha[1] + gram[t, 2] * alpha[2] for t in range(NT)]
        new = [alpha[t] * jnp.exp(-pull[t] / temperature) for t in range(NT)]
        total = new[0] + new[1] + new[2]
        return tuple(a / total for a in new)

    alpha = lax.fori_loop(0, EG_STEPS, eg_step, tuple(alpha))
    small = HALF * LN * 2
    for t in range(NT):
        pack_ref[0:1, small + LN * t:small + LN * (t + 1)] = alpha[t][0:1, :]
        for s in range(NT):
            col = small + LN * (NT + s)
            pack_ref[t:t + 1, col:col + LN] = gram[t, s][0:1, :]
    scale = [jnp.broadcast_to(alpha[t][0:1, :] * inv_tokens, (72, 128)) for t in range(NT)]
    for layer in range(NL):
        u = NT * (NL - 1 - layer)
        mix[72 * layer:72 * (layer + 1), :] = scale[0] * res[u] + scale[1] * res[u + 1] + scale[2] * res[u + 2]
    for k in range(ROWS):
        pack_ref[:, LN * k:LN * (k + 1)] = mix[pl.ds(k, NL, stride=ROWS), :]


def whole_step(x, labels, w_up, w_down, heads_t):
    any_spec = pl.BlockSpec(memory_space=pl.ANY)
    vmem_spec = pl.BlockSpec(memory_space=pltpu.VMEM)
    dma = pltpu.SemaphoreType.DMA
    two, three = (2,), (3,)

    def vmem(*shape, dtype=F32):
        return pltpu.VMEM(shape, dtype)

    both = pltpu.SemaphoreType.DMA(three + three + two)
    triple = dma(three + three + three)
    scratch = [
        vmem(2, DF, TOK, dtype=BF16),
        vmem(2, DM, TOK, dtype=BF16),
        vmem(2, TOK, DF),
        vmem(2, DM, DF, dtype=BF16),
        vmem(2, DF, DM, dtype=BF16),
        vmem(TOK, DM, dtype=BF16),
        vmem(NT, TOK, DM, dtype=BF16),
        vmem(TOK, DF, dtype=BF16),
        vmem(2, 3, DM, LN),
        vmem(3, *GRID, ROWS, LN),
        vmem(2, *GRID, ROWS, LN),
        vmem(2, *GRID, ROWS, LN),
        vmem(3, 3, 2, 2, 4, GRP, LN),
        vmem(3, 3, 2, 4, 4, GRP, LN),
        vmem(3, 3, 4, 4, GRP, LN),
        vmem(3, 3, 2, 2, GRP, LN),
        vmem(3, 3, 2, 4, GRP, LN),
        vmem(3, 3, 4, GRP, LN),
        vmem(3, 3, 3, GRP, LN),
        vmem(UNITS, ROWS, LN),
        vmem(NL * ROWS, LN),
        vmem(8, 8, LN),
        vmem(16, 8, LN),
        dma, dma(two + two), dma(three + two), dma(three + two), dma(two + three), dma(two + three),
        both, both, both, both, both, both, both, both,
        triple, triple, both, both, both, both, dma((7,)), dma((7,)), dma((15,)), dma((15,)),
    ]
    return pl.pallas_call(
        step_kernel,
        out_shape=(
            jax.ShapeDtypeStruct((NL, (ROWS + 2 * NT) * LN), F32),
            jax.ShapeDtypeStruct((2, DF, TOK), BF16),
            jax.ShapeDtypeStruct((2, DM, TOK), BF16),
            jax.ShapeDtypeStruct((2, TOK, DF), F32),
        ),
        in_specs=[any_spec, vmem_spec, any_spec, any_spec, vmem_spec],
        out_specs=(vmem_spec, any_spec, any_spec, any_spec),
        scratch_shapes=scratch,
        compiler_params=pltpu.CompilerParams(
            collective_id=0, has_side_effects=True, vmem_limit_bytes=67043328),
    )(x, labels, w_up, w_down, heads_t)[0]


def solution(mesh):
    def local_step(x_local, lab_local, w_up, w_down, task_heads):
        heads_t = jnp.pad(jnp.swapaxes(task_heads, 1, 2), ((0, 0), (0, 16 - NC), (0, 0))).reshape(NT * 16, DM)
        pack = whole_step(x_local, lab_local, w_up, w_down, heads_t)
        half, small = HALF * LN, 2 * HALF * LN
        alpha = pack[0, small:small + NT * LN:LN]
        gram = pack[:NT, small + NT * LN::LN]
        return alpha, gram, pack[:, :half], pack[:, half:small]

    return jax.shard_map(local_step, mesh=mesh, in_specs=(P('data', None), P(None, 'data'), P(), P(), P()), out_specs=(P(), P(), P(None, 'data'), P(None, 'data')), check_vma=False)
```
